32 devices in a mesh: aa: 8 (over z, y), ba: 4 (over x, core).
Axes of the slice: x: 2, y: 2, z: 4, core: 2. Of those that a mesh axis runs over, the one named last changes fastest.
Arguments:
- tokens: bfloat16 [4096, 8192], P('aa', 'ba'), may hold values from -6 to 6
- request_adapter_index: int32 [4096, 1], P('aa'), may hold values from 0 to 127; in each aligned block of 512 rows (0 to 511, 512 to 1023, ...) at most 8 rows name the same one
- key_weight: bfloat16 [8192, 1024], P('ba'), may hold values from -0.0625 to 0.0625
- value_weight: bfloat16 [8192, 1024], P('ba'), may hold values from -0.0625 to 0.0625
- adapter_down_weight: bfloat16 [128, 32, 8192], P('aa', None, 'ba'), may hold values from -0.0625 to 0.0625
- adapter_up_weight: bfloat16 [128, 2, 16, 1024], P('aa'), may hold values from -1.5 to 1.5
Outputs:
- keys_out: bfloat16 [4096, 1024], P('aa', 'ba')
- values_out: bfloat16 [4096, 1024], P('aa', 'ba')
The draws below stay inside these ranges and needn't reach their ends.
Inputs may be any that keep to these rules, and one draw needn't show every extreme that they name: `request_adapter_index`: among the 512 rows of one device no adapter is named more than 8 times, a bound that some block reaches.
All inputs are finite; a program needn't handle non-finite values.
Results may differ from the reference program's by a relative error of at most 0.001.
Values may be sent and summed in bfloat16 or wider, within the bound.
A program may use at most 128 MiB of HBM per device.

```python
import math
import jax
import jax.numpy as jnp
import numpy as np
from jax import lax

MODEL_WIDTH = 8192
KEY_VALUE_WIDTH = 1024
ADAPTER_RANK = 16
ADAPTER_COUNT = 128
TOK_DEV = 512
TOKENS = 4096
ACAP = 8


def block_scale(stream_key, dims, split, least, high):
    gain, own = 1.0, jax.random.fold_in(stream_key, 6)
    for axis_at, blocks in split:
        heights = jnp.exp(jax.random.uniform(jax.random.fold_in(own, axis_at), (blocks,), jnp.float32, least / len(split), high / len(split)))
        gain = gain * jnp.repeat(heights, dims[axis_at] // blocks).reshape([-1 if axis == axis_at else 1 for axis in range(len(dims))])
    return gain


def shared_out(stream_key, own, number, rows, count, top, limit, lean):
    sequence = jax.random.permutation(stream_key, count)
    heavy_load, usual = portions_of(count, rows * top, limit, lean, True), portions_of(count, rows * top, limit, lean, False)
    places = jnp.arange(count)

    def named(tallies, offset_by):
        used = int((tallies > 0).sum())
        fixed = max(1, used // 4)
        shifted = fixed + (places - fixed + offset_by * (used - fixed)) % max(1, count - fixed)
        return jnp.zeros((count,), jnp.int32).at[sequence[jnp.where(places < fixed, places, shifted)]].set(jnp.asarray(tallies, jnp.int32))

    tallies = jnp.where(number % 4 == 0, named(heavy_load, number // 4), named(usual, number - number // 4 - 1))
    mixed = jax.random.permutation(jax.random.fold_in(own, 3), count)
    giver, sink = mixed[0:count // 2 * 2:2], mixed[1:count // 2 * 2:2]
    room = jnp.minimum(tallies[giver] - 1, limit - tallies[sink]) // 2
    room = jnp.where((giver == sequence[0]) | (sink == sequence[0]) | (tallies[sink] == 0), 0, jnp.maximum(room, 0))
    shifted = jax.random.randint(jax.random.fold_in(own, 4), (count // 2,), 0, 1 << 20) % (room + 1)
    tallies = tallies.at[giver].add(-shifted).at[sink].add(shifted)
    labels = jnp.searchsorted(jnp.cumsum(tallies), jnp.arange(rows * top), side="right").astype(jnp.int32)
    listing = labels.reshape(top, rows).T
    listing = listing[jax.random.permutation(jax.random.fold_in(own, 1), rows)]
    offset_by = jax.random.randint(jax.random.fold_in(own, 2), (rows, 1), 0, top)
    return jnp.take_along_axis(listing, (jnp.arange(top)[None, :] + offset_by) % top, axis=1)


def portions_of(number_of, total, reach, slope, full):
    portions = [(1 << 20) // math.isqrt(standing ** slope) + 1 for standing in range(1, number_of + 1)]
    largest = reach if full else min(reach, max(-(-total // number_of), total * portions[0] // sum(portions)))
    least = 1 if total - largest >= number_of - 1 else 0
    counts, rest = [largest] + [least] * (number_of - 1), total - largest - least * (number_of - 1)
    while rest > 0:
        movable = [i for i in range(1, number_of) if counts[i] < largest] or [i for i in range(1, number_of) if counts[i] < reach]
        whole, remaining = sum([portions[i] for i in movable]), rest
        for i in movable:
            addition = min(reach - counts[i], max(1, remaining * portions[i] // whole), rest)
            counts[i] = counts[i] + addition
            rest = rest - addition
    return np.array(counts)


def noise(own_key, extent, deviation, limit, cuts=(), kind=jnp.bfloat16):
    entries = jax.random.normal(own_key, extent, jnp.float32) * deviation
    if len(cuts) > 0:
        entries = block_scale(own_key, extent, cuts, -0.22, 0.18) * entries
    return jnp.clip(entries, min=-limit, max=limit).astype(kind)


def setup_inputs(seed: int = 0) -> dict:
    splits = jax.random.split(jax.random.key(seed), 7)
    tokens = noise(splits[0], (TOKENS, MODEL_WIDTH), 1.0, 6.0, ((0, 8), (1, 4)))
    request_adapter_index_keys = jax.random.split(jax.random.fold_in(splits[1], 1), TOKENS // TOK_DEV)
    request_adapter_index_turns = jax.random.permutation(jax.random.fold_in(splits[1], 3), TOKENS // TOK_DEV)
    request_adapter_index = jax.vmap(lambda own, number: shared_out(jax.random.fold_in(splits[1], 2), own, number, TOK_DEV, ADAPTER_COUNT, 1, ACAP, 2))(request_adapter_index_keys, request_adapter_index_turns).reshape((TOKENS, 1))
    key_weight = noise(splits[2], (MODEL_WIDTH, KEY_VALUE_WIDTH), MODEL_WIDTH ** -0.5, 0.0625, ((0, 4),))
    value_weight = noise(splits[3], (MODEL_WIDTH, KEY_VALUE_WIDTH), MODEL_WIDTH ** -0.5, 0.0625, ((0, 4),))
    adapter_down_weight = noise(splits[4], (ADAPTER_COUNT, 2 * ADAPTER_RANK, MODEL_WIDTH), MODEL_WIDTH ** -0.5, 0.0625, ((0, 8), (2, 4)))
    adapter_up_weight = noise(splits[5], (ADAPTER_COUNT, 2, ADAPTER_RANK, KEY_VALUE_WIDTH), ADAPTER_RANK ** -0.5, 1.5, ((0, 8),))
    return {"tokens": tokens, "request_adapter_index": request_adapter_index, "key_weight": key_weight, "value_weight": value_weight, "adapter_down_weight": adapter_down_weight, "adapter_up_weight": adapter_up_weight}


def reference(tokens, request_adapter_index, key_weight, value_weight, adapter_down_weight, adapter_up_weight):
    base_key = jnp.dot(tokens, key_weight, preferred_element_type=jnp.float32)
    base_value = jnp.dot(tokens, value_weight, preferred_element_type=jnp.float32)
    height = math.gcd(TOKENS, 64)
    token_blocks = tokens.reshape(TOKENS // height, height, MODEL_WIDTH)
    adapter_blocks = request_adapter_index.reshape(TOKENS // height, height)

    def one_block(pair):
        rows, selected_adapter = pair
        down_weight_rows = adapter_down_weight[selected_adapter].astype(jnp.float32)
        up_weight_rows = adapter_up_weight[selected_adapter].astype(jnp.float32)
        rank_sum = jnp.einsum("td,tjd->tj", rows.astype(jnp.float32), down_weight_rows, precision=lax.Precision.HIGHEST)
        key_change = jnp.einsum("tr,trc->tc", rank_sum[:, :ADAPTER_RANK], up_weight_rows[:, 0], precision=lax.Precision.HIGHEST)
        value_change = jnp.einsum("tr,trc->tc", rank_sum[:, ADAPTER_RANK:], up_weight_rows[:, 1], precision=lax.Precision.HIGHEST)
        return key_change, value_change

    key_change, value_change = lax.map(one_block, (token_blocks, adapter_blocks))
    keys_out = (base_key + key_change.reshape(TOKENS, KEY_VALUE_WIDTH)).astype(jnp.bfloat16)
    values_out = (base_value + value_change.reshape(TOKENS, KEY_VALUE_WIDTH)).astype(jnp.bfloat16)
    return keys_out, values_out
```

```python
import functools

import jax
import jax.numpy as jnp
from jax import lax
from jax.experimental import pallas as pl
from jax.experimental.pallas import tpu as pltpu
from jax.sharding import PartitionSpec as P

MESH = pl.DeviceIdType.MESH
LANES = 128
BF16 = jnp.bfloat16
F32 = jnp.float32


def split_two(x):
    hi = x.astype(BF16)
    return hi, (x - hi.astype(F32)).astype(BF16)


def kernel(
    n, m, cap, resident, twice_rank,
    idx_row, tok_hbm, kw_hbm, vw_hbm, down_hbm, up_hbm,
    acc,
    tok, kw, vw, down, up_all, outgoing, recv, rs_send, rs_recv,
    rank_part, rank_in, ret_send, ret_recv,
    load_sem, up_send_sem, up_recv_sem, d_send_sem, d_recv_sem,
    rs_send_sem, rs_recv_sem, p_send_sem, p_recv_sem, r_send_sem, r_recv_sem,
):
    me = lax.axis_index("aa")
    mb = lax.axis_index("ba")
    rows = tok.shape[0]
    kv = acc.shape[1] // 2
    groups = LANES // twice_rank
    quads = resident // groups
    stride = cap * quads
    chunk = resident * cap
    rank = twice_rank // 2

    loads = [
        pltpu.make_async_copy(tok_hbm, tok, load_sem.at[0]),
        pltpu.make_async_copy(
            up_hbm.at[:, pl.ds(pl.multiple_of(mb * kv, LANES), kv)], up_all.at[me], load_sem.at[1]
        ),
        pltpu.make_async_copy(kw_hbm, kw, load_sem.at[2]),
        pltpu.make_async_copy(vw_hbm, vw, load_sem.at[3]),
        pltpu.make_async_copy(down_hbm, down, load_sem.at[4]),
    ]
    for c in loads:
        c.start()

    barrier = pltpu.get_barrier_semaphore()

    def greet_aa(i, _):
        pl.semaphore_signal(barrier, inc=1, device_id={"aa": lax.rem(me + i, n)}, device_id_type=MESH)
        return 0

    def greet_ba(i, _):
        pl.semaphore_signal(barrier, inc=1, device_id={"ba": lax.rem(mb + i, m)}, device_id_type=MESH)
        return 0

    lax.fori_loop(1, n, greet_aa, 0)
    lax.fori_loop(1, m, greet_ba, 0)

    def slot(a, earlier):
        local = lax.rem(a, resident)
        return (a // resident) * chunk + lax.rem(local, groups) * stride + earlier * quads + local // groups

    row = idx_row[...]
    down_pos = lax.broadcasted_iota(jnp.int32, (rows, rows), 0)
    lane_pos = lax.broadcasted_iota(jnp.int32, (rows, rows), 1)
    col = jnp.sum(jnp.where(down_pos == lane_pos, row, 0), axis=1, keepdims=True)
    same = col == row
    slot_col = slot(col, jnp.sum(jnp.where(same & (lane_pos < down_pos), 1, 0), axis=1, keepdims=True))
    slot_row = slot(row, jnp.sum(jnp.where(same & (down_pos < lane_pos), 1, 0), axis=0, keepdims=True))

    def flip(x, b):
        return x + b - 2 * b * lax.rem(x // b, 2)

    bits = []
    bit = n // 2
    while bit:
        bits.append(bit)
        bit //= 2

    far = list(range(n // 2, n))
    near = list(range(n // 4, n // 2))
    order = [0]
    while far:
        if near:
            order.append(near.pop(0))
        order.append(far.pop(0))
    order += near + [d for d in range(n // 4 - 1, 0, -1)]

    def peer(i):
        mask = sum([jnp.where(i == at, order[at], 0) for at in range(1, n)], jnp.int32(0))
        other = me
        for b in bits:
            other = jnp.where(lax.rem(mask // b, 2) == 1, flip(other, b), other)
        return other

    def dispatch(i):
        return pltpu.make_async_remote_copy(
            src_ref=outgoing.at[i], dst_ref=recv.at[i],
            send_sem=d_send_sem.at[i], recv_sem=d_recv_sem.at[i],
            device_id={"aa": peer(i)}, device_id_type=MESH,
        )

    def fill(i):
        wanted = lax.broadcasted_iota(jnp.int32, (chunk, rows), 0) + peer(i) * chunk
        pick = jnp.where(wanted == slot_row, 1.0, 0.0).astype(BF16)
        return jnp.dot(pick, tok[...], preferred_element_type=F32).astype(BF16)

    up_copies = []
    held = [()]
    number = 0
    for b in bits:
        stage = []
        for path in held:
            block = me
            for q in path:
                block = flip(block, q)
            stage.append((block, flip(me, b), number))
            number += 1
        up_copies.append(stage)
        held = held + [path + (b,) for path in held]

    def up_copy(block, partner, at):
        return pltpu.make_async_remote_copy(
            src_ref=up_all.at[block], dst_ref=up_all.at[block],
            send_sem=up_send_sem.at[at], recv_sem=up_recv_sem.at[at],
            device_id={"aa": partner}, device_id_type=MESH,
        )

    pl.semaphore_wait(barrier, n + m - 2)
    loads[1].wait()
    loads[0].wait()

    def send_one(i, _):
        outgoing[i] = fill(i)
        dispatch(i).start()
        return 0

    def up_stage(at):
        if at > 0:
            for entry in up_copies[at - 1]:
                up_copy(*entry).wait_recv()
        if at < len(up_copies):
            for entry in up_copies[at]:
                up_copy(*entry).start()

    up_stage(0)
    lax.fori_loop(1, 3, send_one, 0)

    loads[2].wait()
    loads[3].wait()

    def rs_copy(b):
        return pltpu.make_async_remote_copy(
            src_ref=rs_send.at[b], dst_ref=rs_recv.at[b],
            send_sem=rs_send_sem.at[b], recv_sem=rs_recv_sem.at[b],
            device_id={"ba": lax.rem(mb + b + 1, m)}, device_id_type=MESH,
        )

    def base(b, _):
        cols = pl.ds(pl.multiple_of(lax.rem(mb + b + 1, m) * kv, LANES), kv)
        rs_send[b, :, :kv] = jnp.dot(tok[...], kw[:, cols], preferred_element_type=F32)
        rs_send[b, :, kv:] = jnp.dot(tok[...], vw[:, cols], preferred_element_type=F32)

        @pl.when(b < m - 1)
        def _():
            rs_copy(b).start()

        return 0

    lax.fori_loop(0, m // 2, base, 0)
    up_stage(1)
    lax.fori_loop(3, 5, send_one, 0)
    lax.fori_loop(m // 2, m, base, 0)
    recv[0] = fill(0)
    up_stage(2)
    lax.fori_loop(5, n, send_one, 0)
    loads[4].wait()

    def add_part(b, _):
        rs_copy(b).wait_recv()
        rs_send[m - 1] += rs_recv[b]
        return 0

    width = resident * twice_rank
    slot_of_row = lax.broadcasted_iota(jnp.int32, (chunk, width), 0)
    column = lax.broadcasted_iota(jnp.int32, (chunk, width), 1)
    adapter_of_row = lax.rem(slot_of_row, quads) * groups + slot_of_row // stride
    own = adapter_of_row == column // twice_rank
    for_key = lax.rem(column, twice_rank) < rank

    def part_copy(b, i):
        return pltpu.make_async_remote_copy(
            src_ref=rank_part.at[i], dst_ref=rank_in.at[b, i],
            send_sem=p_send_sem.at[b, i], recv_sem=p_recv_sem.at[b, i],
            device_id={"ba": lax.rem(mb + b + 1, m)}, device_id_type=MESH,
        )

    def ret_copy(i):
        return pltpu.make_async_remote_copy(
            src_ref=ret_send.at[i], dst_ref=ret_recv.at[i],
            send_sem=r_send_sem.at[i], recv_sem=r_recv_sem.at[i],
            device_id={"aa": peer(i)}, device_id_type=MESH,
        )

    def partial(i):
        @pl.when(i > 0)
        def _():
            dispatch(i).wait_recv()

        wide = lax.dot_general(
            recv[i], down[...], (((1,), (1,)), ((), ())), preferred_element_type=F32
        )
        wide = jnp.where(own, wide, 0.0)
        total = wide[:, :LANES]
        for q in range(1, width // LANES):
            total = total + wide[:, q * LANES:(q + 1) * LANES]
        packed = total[:stride]
        for g in range(1, groups):
            packed = packed + total[g * stride:(g + 1) * stride]
        rank_part[i] = packed
        for b in range(m - 1):
            part_copy(b, i).start()

    def finish(i):
        total = rank_part[i]
        for b in range(m - 1):
            part_copy(b, i).wait_recv()
            total = total + rank_in[b, i]

        @pl.when(i == 0)
        def _():
            ret_recv[i] = total

        @pl.when(i > 0)
        def _():
            ret_send[i] = total
            ret_copy(i).start()

    def final(i):
        @pl.when(i > 0)
        def _():
            ret_copy(i).wait_recv()

        tall = jnp.concatenate([ret_recv[i]] * groups, axis=0)
        spread = jnp.where(own, jnp.concatenate([tall] * (width // LANES), axis=1), 0.0)
        key_hi, key_lo = split_two(jnp.where(for_key, spread, 0.0))
        value_hi, value_lo = split_two(jnp.where(for_key, 0.0, spread))
        bank = peer(i)
        up = up_all[bank]
        pieces = jnp.concatenate([key_hi, key_lo, value_hi, value_lo], axis=0)
        out = jnp.dot(pieces, up, preferred_element_type=F32)
        change = jnp.concatenate(
            [out[:chunk] + out[chunk:2 * chunk], out[2 * chunk:3 * chunk] + out[3 * chunk:]], axis=1
        )
        hi, lo = split_two(change)
        place = lax.broadcasted_iota(jnp.int32, (rows, chunk), 1) + bank * chunk
        pick = jnp.where(place == slot_col, 1.0, 0.0).astype(BF16)
        acc[...] += jnp.dot(pick, hi, preferred_element_type=F32) + jnp.dot(
            pick, lo, preferred_element_type=F32
        )

    def step(t, _):
        @pl.when((t >= 1) & (t < n + 1))
        def _():
            finish(t - 1)

        @pl.when(t == 2)
        def _():
            for at in range(3, len(up_copies) + 1):
                up_stage(at)
            lax.fori_loop(0, m - 1, add_part, 0)
            acc[...] = rs_send[m - 1]

        @pl.when(t >= 2)
        def _():
            final(t - 2)

        @pl.when(t < n)
        def _():
            partial(t)

        return 0

    lax.fori_loop(0, n + 2, step, 0)

    for stage in up_copies:
        for entry in stage:
            up_copy(*entry).wait_send()

    def drain(i, _):
        dispatch(i).wait_send()
        ret_copy(i).wait_send()
        return 0

    lax.fori_loop(1, n, drain, 0)

    def drain_parts(i, _):
        for b in range(m - 1):
            part_copy(b, i).wait_send()
        return 0

    lax.fori_loop(0, n, drain_parts, 0)
    for b in range(m - 1):
        rs_copy(b).wait_send()


def xor_bit(x, b):
    return x + b - 2 * b * lax.rem(x // b, 2)


def bits_of(count):
    found = []
    bit = count // 2
    while bit:
        found.append(bit)
        bit //= 2
    return found


def low_bit(mask):
    return mask & -mask


def packed_kernel(
    n, m, direct, shared, near_rows, stride, resident, twice_rank,
    idx_hbm, tok_hbm, kw_hbm, vw_hbm, down_hbm, up_hbm,
    keys, values, flag,
    idx_mine, idx_all, mine, tri, tok, kw, vw, down, up_all, shared_out, outgoing, recv,
    rs_send, rs_recv, acc, rank_part, rank_in, ret_send, ret_recv,
    load_sem, idx_send_sem, idx_recv_sem, up_send_sem, up_recv_sem, v_send_sem, v_recv_sem,
    d_send_sem, d_recv_sem, rs_send_sem, rs_recv_sem, p_send_sem, p_recv_sem, r_send_sem, r_recv_sem,
):
    me = lax.axis_index("aa")
    mb = lax.axis_index("ba")
    rows = tok.shape[0]
    kv = keys.shape[1]
    half = n // 2
    slots = direct + shared
    groups = LANES // twice_rank
    packed = rank_part.shape[1]
    rank = twice_rank // 2
    width = resident * twice_rank
    bits = bits_of(n)
    ba_bits = bits_of(m)[::-1]
    count = jnp.int32

    barrier = pltpu.get_barrier_semaphore()

    def greet_aa(i, _):
        pl.semaphore_signal(barrier, inc=1, device_id={"aa": lax.rem(me + i, n)}, device_id_type=MESH)
        return 0

    def greet_ba(i, _):
        pl.semaphore_signal(barrier, inc=1, device_id={"ba": lax.rem(mb + i, m)}, device_id_type=MESH)
        return 0

    lax.fori_loop(1, n, greet_aa, 0)
    lax.fori_loop(1, m, greet_ba, 0)

    loads = [
        pltpu.make_async_copy(idx_hbm, idx_mine, load_sem.at[0]),
        pltpu.make_async_copy(
            up_hbm.at[:, pl.ds(pl.multiple_of(mb * kv, LANES), kv)], up_all.at[0], load_sem.at[1]
        ),
        pltpu.make_async_copy(tok_hbm, tok, load_sem.at[2]),
        pltpu.make_async_copy(kw_hbm, kw, load_sem.at[3]),
        pltpu.make_async_copy(vw_hbm, vw, load_sem.at[4]),
        pltpu.make_async_copy(down_hbm, down, load_sem.at[5]),
    ]
    for c in loads:
        c.start()

    def partner(mask):
        other = me
        for b in bits:
            other = jnp.where(lax.rem(mask // b, 2) == 1, xor_bit(other, b), other)
        return other

    def chosen(masks, t):
        return sum([jnp.where(t == at, mask, 0) for at, mask in enumerate(masks)], jnp.int32(0))

    def idx_copy(mask, source):
        return pltpu.make_async_remote_copy(
            src_ref=idx_mine, dst_ref=idx_all.at[source],
            send_sem=idx_send_sem.at[mask], recv_sem=idx_recv_sem.at[mask],
            device_id={"aa": partner(mask)}, device_id_type=MESH,
        )

    def up_copy(mask):
        hop = low_bit(mask)
        return pltpu.make_async_remote_copy(
            src_ref=up_all.at[mask - hop], dst_ref=up_all.at[mask],
            send_sem=up_send_sem.at[mask], recv_sem=up_recv_sem.at[mask],
            device_id={"aa": xor_bit(me, hop)}, device_id_type=MESH,
        )

    def shared_copy(mask):
        hop = low_bit(mask)
        source = shared_out if mask == half else recv.at[mask - hop, pl.ds(direct, shared)]
        return pltpu.make_async_remote_copy(
            src_ref=source, dst_ref=recv.at[mask, pl.ds(direct, shared)],
            send_sem=v_send_sem.at[mask], recv_sem=v_recv_sem.at[mask],
            device_id={"aa": xor_bit(me, hop)}, device_id_type=MESH,
        )

    def row_copy(mask, height):
        return pltpu.make_async_remote_copy(
            src_ref=outgoing.at[mask, pl.ds(0, height)], dst_ref=recv.at[mask, pl.ds(0, height)],
            send_sem=d_send_sem.at[mask], recv_sem=d_recv_sem.at[mask],
            device_id={"aa": partner(mask)}, device_id_type=MESH,
        )

    def hops_below(mask):
        return [b for b in bits if b < low_bit(mask)]

    earlier = lax.broadcasted_iota(count, (rows, rows), 0)
    later = lax.broadcasted_iota(count, (rows, rows), 1)
    tri[...] = jnp.where(earlier < later, 1.0, 0.0).astype(BF16)
    loads[0].wait()
    row = idx_mine[...]
    bank_row = row // resident
    tall = max(16, n)
    match = lax.broadcasted_iota(count, (tall, rows), 0) == bank_row
    ranks = jnp.dot(jnp.where(match, 1.0, 0.0).astype(BF16), tri[...], preferred_element_type=F32)
    rank_row = jnp.sum(jnp.where(match, ranks, 0.0), axis=0, keepdims=True).astype(count)
    far_row = (bank_row // half) != (me // half)
    over_row = jnp.where(far_row & (rank_row >= direct), 1.0, 0.0)
    over_rank = jnp.dot(
        jnp.broadcast_to(over_row, (tall, rows)).astype(BF16), tri[...], preferred_element_type=F32
    )[:1].astype(count)
    slot_row = jnp.where(over_row > 0.5, direct + over_rank, rank_row)
    code_row = bank_row * stride + slot_row
    shared_row = jnp.where(over_row > 0.5, over_rank, -1)

    def gathered(wanted, at):
        pick = jnp.where(wanted == at, 1.0, 0.0).astype(BF16)
        return jnp.dot(pick, tok[...], preferred_element_type=F32).astype(BF16)

    def fill(bank, height):
        return gathered(lax.broadcasted_iota(count, (height, rows), 0) + bank * stride, code_row)

    pl.semaphore_wait(barrier, n + m - 2)

    def send_idx(mask, _):
        idx_copy(mask, me).start()
        return 0

    lax.fori_loop(1, n, send_idx, 0)
    loads[1].wait()
    for b in bits:
        if b != half // 2:
            up_copy(b).start()
    loads[2].wait()
    shared_out[...] = gathered(lax.broadcasted_iota(count, (shared, rows), 0), shared_row)
    shared_copy(half).start()
    if half > 1:
        up_copy(half // 2).start()

    near = sorted(range(1, half), key=lambda mask: (-low_bit(mask) * 0 - mask // 2, mask))
    far = sorted(range(half, n), key=lambda mask: (mask % 2, mask))

    def send_near(t, _):
        mask = chosen(near, t)
        outgoing[mask] = fill(partner(mask), near_rows)
        row_copy(mask, near_rows).start()
        return 0

    def send_far(t, _):
        mask = chosen(far, t)
        outgoing[mask, pl.ds(0, direct)] = fill(partner(mask), direct)
        row_copy(mask, direct).start()
        return 0

    lax.fori_loop(0, len(near), send_near, 0)
    first = len(far) // 2
    lax.fori_loop(0, first, send_far, 0)

    def rs_copy(q):
        hop = low_bit(q)
        return pltpu.make_async_remote_copy(
            src_ref=rs_send.at[q], dst_ref=rs_recv.at[q],
            send_sem=rs_send_sem.at[q], recv_sem=rs_recv_sem.at[q],
            device_id={"ba": xor_bit(mb, hop)}, device_id_type=MESH,
        )

    loads[3].wait()
    loads[4].wait()
    base_order = sorted(range(1, m), key=lambda q: (low_bit(q), q)) + [0]

    def base(t, _):
        q = chosen(base_order, t)
        block = mb
        for b in ba_bits:
            block = jnp.where(lax.rem(q // b, 2) == 1, xor_bit(block, b), block)
        cols = pl.ds(pl.multiple_of(block * kv, LANES), kv)
        rs_send[q, :, :kv] = jnp.dot(tok[...], kw[:, cols], preferred_element_type=F32)
        rs_send[q, :, kv:] = jnp.dot(tok[...], vw[:, cols], preferred_element_type=F32)
        for at, q_now in enumerate(base_order):
            if q_now:
                @pl.when(t == at)
                def _():
                    for b in ba_bits:
                        if b < low_bit(q_now):
                            rs_copy(q_now + b).wait_recv()
                            rs_send[q_now] += rs_recv[q_now + b]
                    rs_copy(q_now).start()

        return 0

    lax.fori_loop(0, m, base, 0)

    idx_all[me] = row
    for_self = fill(me, near_rows)
    recv[0, pl.ds(0, near_rows)] = for_self
    for mask in range(half):
        recv[mask, pl.ds(near_rows, slots - near_rows)] = jnp.zeros((slots - near_rows, tok.shape[1]), BF16)

    def wait_idx(mask, _):
        idx_copy(mask, partner(mask)).wait_recv()
        return 0

    lax.fori_loop(1, n, wait_idx, 0)
    everyone = jnp.concatenate([idx_all[s] for s in range(n)], axis=0)
    banks = everyone // resident
    matches = [banks == b for b in range(n)]
    stacked = jnp.concatenate([jnp.where(hit, 1.0, 0.0) for hit in matches], axis=0)
    all_ranks = jnp.dot(stacked.astype(BF16), tri[...], preferred_element_type=F32)
    place = jnp.zeros((n, rows), F32)
    for b in range(n):
        place = place + jnp.where(matches[b], all_ranks[b * n:(b + 1) * n], 0.0)
    place = place.astype(count)
    far_all = (banks // half) != (lax.broadcasted_iota(count, (n, rows), 0) // half)
    over_all = jnp.where(far_all & (place >= direct), 1.0, 0.0)
    padded = jnp.concatenate([over_all] * (tall // n), axis=0)
    over_ranks = jnp.dot(padded.astype(BF16), tri[...], preferred_element_type=F32)[:n].astype(count)
    place = jnp.where(over_all > 0.5, direct + over_ranks, place)
    excess = jnp.where(place >= jnp.where(far_all, slots, near_rows), 1, 0)
    flag[...] = jnp.broadcast_to(
        jnp.max(jnp.max(excess, axis=1, keepdims=True), axis=0, keepdims=True), flag.shape
    )
    to_me = jnp.where(banks == me, place, -1)
    for s in range(n):
        mine[s] = to_me[s:s + 1]
    code_col = jnp.sum(jnp.where(earlier == later, code_row, 0), axis=1, keepdims=True)

    lane = lax.broadcasted_iota(count, (packed, LANES), 1) // twice_rank
    column = lax.broadcasted_iota(count, (slots, width), 1)
    for_key = lax.rem(column, twice_rank) < rank

    def folded(x):
        total = x
        for g in range(1, groups):
            total = total + pltpu.roll(x, g * twice_rank, axis=1)
        return total

    def owned(wanted, at, ids):
        local = jnp.sum(jnp.where(wanted == at, lax.rem(ids, resident), 0), axis=1, keepdims=True)
        return local == column // twice_rank

    def part_copy(b, mask):
        return pltpu.make_async_remote_copy(
            src_ref=rank_part.at[mask], dst_ref=rank_in.at[b, mask],
            send_sem=p_send_sem.at[b, mask], recv_sem=p_recv_sem.at[b, mask],
            device_id={"ba": lax.rem(mb + b + 1, m)}, device_id_type=MESH,
        )

    def ret_copy(mask):
        return pltpu.make_async_remote_copy(
            src_ref=ret_send.at[mask], dst_ref=ret_recv.at[mask],
            send_sem=r_send_sem.at[mask], recv_sem=r_recv_sem.at[mask],
            device_id={"aa": partner(mask)}, device_id_type=MESH,
        )

    def partial(mask):
        @pl.when((mask > 0) & (mask < half))
        def _():
            row_copy(mask, near_rows).wait_recv()

        @pl.when(mask >= half)
        def _():
            row_copy(mask, direct).wait_recv()

        source = partner(mask)
        wide = lax.dot_general(
            recv[mask], down[...], (((1,), (1,)), ((), ())), preferred_element_type=F32
        )
        own = owned(lax.broadcasted_iota(count, (slots, rows), 0), mine[source], idx_all[source])
        wide = jnp.where(own, wide, 0.0)
        total = wide[:, :LANES]
        for q in range(1, width // LANES):
            total = total + wide[:, q * LANES:(q + 1) * LANES]
        total = folded(total)
        if groups * packed > slots:
            total = jnp.concatenate([total, jnp.zeros((groups * packed - slots, LANES), F32)], axis=0)
        together = total[:packed]
        for g in range(1, groups):
            together = jnp.where(lane == g, total[g * packed:(g + 1) * packed], together)
        rank_part[mask] = together
        for b in range(m - 1):
            part_copy(b, mask).start()

    def finish(mask):
        total = rank_part[mask]
        for b in range(m - 1):
            part_copy(b, mask).wait_recv()
            total = total + rank_in[b, mask]

        @pl.when(mask == 0)
        def _():
            ret_recv[mask] = total

        @pl.when(mask > 0)
        def _():
            ret_send[mask] = total
            ret_copy(mask).start()

    def final(mask):
        @pl.when(mask > 0)
        def _():
            ret_copy(mask).wait_recv()

        bank = partner(mask)
        together = ret_recv[mask]
        tall_ranks = jnp.concatenate(
            [folded(jnp.where(lane == g, together, 0.0)) for g in range(groups)], axis=0
        )[:slots]
        own = owned(lax.broadcasted_iota(count, (slots, rows), 0) + bank * stride, code_row, row)
        spread = jnp.where(own, jnp.concatenate([tall_ranks] * (width // LANES), axis=1), 0.0)
        key_hi, key_lo = split_two(jnp.where(for_key, spread, 0.0))
        value_hi, value_lo = split_two(jnp.where(for_key, 0.0, spread))
        pieces = jnp.concatenate([key_hi, key_lo, value_hi, value_lo], axis=0)
        out = jnp.dot(pieces, up_all[mask], preferred_element_type=F32)
        change = jnp.concatenate(
            [out[:slots] + out[slots:2 * slots], out[2 * slots:3 * slots] + out[3 * slots:]], axis=1
        )
        hi, lo = split_two(change)
        pick = jnp.where(
            lax.broadcasted_iota(count, (rows, slots), 1) + bank * stride == code_col, 1.0, 0.0
        ).astype(BF16)
        acc[...] += jnp.dot(pick, hi, preferred_element_type=F32) + jnp.dot(
            pick, lo, preferred_element_type=F32
        )

    order = [0] + sorted(range(1, half), key=lambda mask: (mask // 2, mask)) + far
    loads[5].wait()

    def relay_up(mask):
        up_copy(mask).wait_recv()
        for b in hops_below(mask):
            up_copy(mask + b).start()

    def relay_shared(mask):
        shared_copy(mask).wait_recv()
        for b in hops_below(mask):
            shared_copy(mask + b).start()

    def step(t, _):
        @pl.when((t >= 1) & (t < n + 1))
        def _():
            finish(chosen(order, t - 1))

        for at, mask in enumerate(order):
            if mask and mask != half and mask % 2 == 0 or mask > half:
                @pl.when(t == at)
                def _():
                    if mask % 2 == 0:
                        relay_up(mask)
                    if mask > half:
                        relay_shared(mask)

        @pl.when(t == 2)
        def _():
            for b in ba_bits:
                rs_copy(b).wait_recv()
                rs_send[0] += rs_recv[b]
            acc[...] = rs_send[0]

        @pl.when(t >= 2)
        def _():
            for at, mask in enumerate(order):
                if mask % 2:
                    @pl.when(t == at + 2)
                    def _():
                        up_copy(mask).wait_recv()

            final(chosen(order, t - 2))

        @pl.when(t < n)
        def _():
            partial(chosen(order, t))

        return 0

    lax.fori_loop(0, 2, step, 0)
    relay_up(half)
    lax.fori_loop(first, len(far) - 1, send_far, 0)
    relay_shared(half)
    lax.fori_loop(len(far) - 1, len(far), send_far, 0)
    lax.fori_loop(2, n + 2, step, 0)
    keys[...] = acc[:, :kv].astype(BF16)
    values[...] = acc[:, kv:].astype(BF16)

    for mask in range(1, n):
        up_copy(mask).wait_send()
    for mask in range(half, n):
        shared_copy(mask).wait_send()

    def drain(mask, _):
        idx_copy(mask, me).wait_send()
        ret_copy(mask).wait_send()

        @pl.when(mask < half)
        def _():
            row_copy(mask, near_rows).wait_send()

        @pl.when(mask >= half)
        def _():
            row_copy(mask, direct).wait_send()

        return 0

    lax.fori_loop(1, n, drain, 0)

    def drain_parts(mask, _):
        for b in range(m - 1):
            part_copy(b, mask).wait_send()
        return 0

    lax.fori_loop(0, n, drain_parts, 0)
    for q in range(1, m):
        rs_copy(q).wait_send()


def packed_call(n, m, cap, idx, tokens, key_weight, value_weight, down_flat, up_flat, resident):
    rows, width = tokens.shape
    flat = down_flat.shape[0]
    twice_rank = flat // resident
    kv_width = key_weight.shape[1]
    kv = kv_width // m
    direct = rows // n
    shared = 3 * direct // 4
    near_rows = 3 * direct // 2
    slots = direct + shared
    stride = resident * cap
    packed = stride * twice_rank // LANES
    dma = pltpu.SemaphoreType.DMA
    return pl.pallas_call(
        functools.partial(packed_kernel, n, m, direct, shared, near_rows, stride, resident, twice_rank),
        out_shape=[
            jax.ShapeDtypeStruct((rows, kv), BF16),
            jax.ShapeDtypeStruct((rows, kv), BF16),
            jax.ShapeDtypeStruct((8, LANES), jnp.int32),
        ],
        in_specs=[pl.BlockSpec(memory_space=pl.ANY)] * 6,
        out_specs=[pl.BlockSpec(memory_space=pltpu.VMEM)] * 3,
        scratch_shapes=[
            pltpu.VMEM((1, rows), jnp.int32),
            pltpu.VMEM((n, 1, rows), jnp.int32),
            pltpu.VMEM((n, 1, rows), jnp.int32),
            pltpu.VMEM((rows, rows), BF16),
            pltpu.VMEM((rows, width), BF16),
            pltpu.VMEM((width, kv_width), BF16),
            pltpu.VMEM((width, kv_width), BF16),
            pltpu.VMEM((flat, width), BF16),
            pltpu.VMEM((n, flat, kv), BF16),
            pltpu.VMEM((shared, width), BF16),
            pltpu.VMEM((n, near_rows, width), BF16),
            pltpu.VMEM((n, slots, width), BF16),
            pltpu.VMEM((m, rows, 2 * kv), F32),
            pltpu.VMEM((m, rows, 2 * kv), F32),
            pltpu.VMEM((rows, 2 * kv), F32),
            pltpu.VMEM((n, packed, LANES), F32),
            pltpu.VMEM((m - 1, n, packed, LANES), F32),
            pltpu.VMEM((n, packed, LANES), F32),
            pltpu.VMEM((n, packed, LANES), F32),
            dma((6,)),
            dma((n,)), dma((n,)), dma((n,)), dma((n,)), dma((n,)), dma((n,)),
            dma((n,)), dma((n,)),
            dma((m,)), dma((m,)),
            dma((m - 1, n)), dma((m - 1, n)),
            dma((n,)), dma((n,)),
        ],
        compiler_params=pltpu.CompilerParams(
            collective_id=1, has_side_effects=True, vmem_limit_bytes=56 * 1024 * 1024
        ),
    )(idx, tokens, key_weight, value_weight, down_flat, up_flat)


def on_device(n, m, tokens, request_adapter_index, key_weight, value_weight, down_weight, up_weight):
    rows, width = tokens.shape
    resident, twice_rank, _ = down_weight.shape
    kv_width = key_weight.shape[1]
    kv = kv_width // m
    cap = max(2, 2 * rows // (resident * n))
    chunk = resident * cap
    packed = chunk * twice_rank // LANES
    flat = resident * twice_rank
    operands = (
        request_adapter_index.reshape(1, rows),
        tokens,
        key_weight,
        value_weight,
        down_weight.reshape(flat, width),
        up_weight.reshape(flat, kv_width),
    )

    def any_load():
        dma = pltpu.SemaphoreType.DMA
        total = pl.pallas_call(
            functools.partial(kernel, n, m, cap, resident, twice_rank),
            out_shape=jax.ShapeDtypeStruct((rows, 2 * kv), F32),
            in_specs=[pl.BlockSpec(memory_space=pltpu.VMEM)] + [pl.BlockSpec(memory_space=pl.ANY)] * 5,
            out_specs=pl.BlockSpec(memory_space=pltpu.VMEM),
            scratch_shapes=[
                pltpu.VMEM((rows, width), BF16),
                pltpu.VMEM((width, kv_width), BF16),
                pltpu.VMEM((width, kv_width), BF16),
                pltpu.VMEM((flat, width), BF16),
                pltpu.VMEM((n, flat, kv), BF16),
                pltpu.VMEM((n, chunk, width), BF16),
                pltpu.VMEM((n, chunk, width), BF16),
                pltpu.VMEM((m, rows, 2 * kv), F32),
                pltpu.VMEM((m - 1, rows, 2 * kv), F32),
                pltpu.VMEM((n, packed, LANES), F32),
                pltpu.VMEM((m - 1, n, packed, LANES), F32),
                pltpu.VMEM((n, packed, LANES), F32),
                pltpu.VMEM((n, packed, LANES), F32),
                dma((5,)),
                dma((n,)), dma((n,)), dma((n,)), dma((n,)),
                dma((m,)), dma((m,)),
                dma((m - 1, n)), dma((m - 1, n)),
                dma((n,)), dma((n,)),
            ],
            compiler_params=pltpu.CompilerParams(
                collective_id=0, has_side_effects=True, vmem_limit_bytes=56 * 1024 * 1024
            ),
        )(
            *operands,
        )
        return total[:, :kv].astype(BF16), total[:, kv:].astype(BF16)

    if rows % (64 * n) or 7 * rows // (4 * n) >= chunk:
        return any_load()
    keys, values, flag = packed_call(n, m, cap, *operands, resident)
    return lax.cond(flag[0, 0] > 0, any_load, lambda: (keys, values))


def solution(mesh):
    return jax.shard_map(
        functools.partial(on_device, mesh.shape["aa"], mesh.shape["ba"]),
        mesh=mesh,
        in_specs=(
            P("aa", "ba"),
            P("aa", None),
            P("ba", None),
            P("ba", None),
            P("aa", None, "ba"),
            P("aa", None, None, None),
        ),
        out_specs=(P("aa", "ba"), P("aa", "ba")),
        check_vma=False,
    )
```

```python
import functools

import jax
import jax.numpy as jnp
from jax import lax
from jax.experimental import pallas as pl
from jax.experimental.pallas import tpu as pltpu
from jax.sharding import PartitionSpec as P

MESH = pl.DeviceIdType.MESH
LANES = 128
BF16 = jnp.bfloat16
F32 = jnp.float32


def split_two(x):
    hi = x.astype(BF16)
    return hi, (x - hi.astype(F32)).astype(BF16)


def kernel(
    n, m, cap, resident, twice_rank,
    idx_row, tok_hbm, kw_hbm, vw_hbm, down_hbm, up_hbm,
    acc,
    tok, kw, vw, down, up_all, outgoing, recv, rs_send, rs_recv,
    rank_part, rank_in, ret_send, ret_recv,
    load_sem, up_send_sem, up_recv_sem, d_send_sem, d_recv_sem,
    rs_send_sem, rs_recv_sem, p_send_sem, p_recv_sem, r_send_sem, r_recv_sem,
):
    me = lax.axis_index("aa")
    mb = lax.axis_index("ba")
    rows = tok.shape[0]
    kv = acc.shape[1] // 2
    groups = LANES // twice_rank
    quads = resident // groups
    stride = cap * quads
    chunk = resident * cap
    rank = twice_rank // 2

    loads = [
        pltpu.make_async_copy(tok_hbm, tok, load_sem.at[0]),
        pltpu.make_async_copy(
            up_hbm.at[:, pl.ds(pl.multiple_of(mb * kv, LANES), kv)], up_all.at[me], load_sem.at[1]
        ),
        pltpu.make_async_copy(kw_hbm, kw, load_sem.at[2]),
        pltpu.make_async_copy(vw_hbm, vw, load_sem.at[3]),
        pltpu.make_async_copy(down_hbm, down, load_sem.at[4]),
    ]
    for c in loads:
        c.start()

    barrier = pltpu.get_barrier_semaphore()

    def greet_aa(i, _):
        pl.semaphore_signal(barrier, inc=1, device_id={"aa": lax.rem(me + i, n)}, device_id_type=MESH)
        return 0

    def greet_ba(i, _):
        pl.semaphore_signal(barrier, inc=1, device_id={"ba": lax.rem(mb + i, m)}, device_id_type=MESH)
        return 0

    lax.fori_loop(1, n, greet_aa, 0)
    lax.fori_loop(1, m, greet_ba, 0)

    def slot(a, earlier):
        local = lax.rem(a, resident)
        return (a // resident) * chunk + lax.rem(local, groups) * stride + earlier * quads + local // groups

    row = idx_row[...]
    down_pos = lax.broadcasted_iota(jnp.int32, (rows, rows), 0)
    lane_pos = lax.broadcasted_iota(jnp.int32, (rows, rows), 1)
    col = jnp.sum(jnp.where(down_pos == lane_pos, row, 0), axis=1, keepdims=True)
    same = col == row
    slot_col = slot(col, jnp.sum(jnp.where(same & (lane_pos < down_pos), 1, 0), axis=1, keepdims=True))
    slot_row = slot(row, jnp.sum(jnp.where(same & (down_pos < lane_pos), 1, 0), axis=0, keepdims=True))

    def flip(x, b):
        return x + b - 2 * b * lax.rem(x // b, 2)

    bits = []
    bit = n // 2
    while bit:
        bits.append(bit)
        bit //= 2

    far = list(range(n // 2, n))
    near = list(range(n // 4, n // 2))
    order = [0]
    while far:
        if near:
            order.append(near.pop(0))
        order.append(far.pop(0))
    order += near + [d for d in range(n // 4 - 1, 0, -1)]

    def peer(i):
        mask = sum([jnp.where(i == at, order[at], 0) for at in range(1, n)], jnp.int32(0))
        other = me
        for b in bits:
            other = jnp.where(lax.rem(mask // b, 2) == 1, flip(other, b), other)
        return other

    def dispatch(i):
        return pltpu.make_async_remote_copy(
            src_ref=outgoing.at[i], dst_ref=recv.at[i],
            send_sem=d_send_sem.at[i], recv_sem=d_recv_sem.at[i],
            device_id={"aa": peer(i)}, device_id_type=MESH,
        )

    def fill(i):
        wanted = lax.broadcasted_iota(jnp.int32, (chunk, rows), 0) + peer(i) * chunk
        pick = jnp.where(wanted == slot_row, 1.0, 0.0).astype(BF16)
        return jnp.dot(pick, tok[...], preferred_element_type=F32).astype(BF16)

    up_copies = []
    held = [()]
    number = 0
    for b in bits:
        stage = []
        for path in held:
            block = me
            for q in path:
                block = flip(block, q)
            stage.append((block, flip(me, b), number))
            number += 1
        up_copies.append(stage)
        held = held + [path + (b,) for path in held]

    def up_copy(block, partner, at):
        return pltpu.make_async_remote_copy(
            src_ref=up_all.at[block], dst_ref=up_all.at[block],
            send_sem=up_send_sem.at[at], recv_sem=up_recv_sem.at[at],
            device_id={"aa": partner}, device_id_type=MESH,
        )

    pl.semaphore_wait(barrier, n + m - 2)
    loads[1].wait()
    loads[0].wait()

    def send_one(i, _):
        outgoing[i] = fill(i)
        dispatch(i).start()
        return 0

    def up_stage(at):
        if at > 0:
            for entry in up_copies[at - 1]:
                up_copy(*entry).wait_recv()
        if at < len(up_copies):
            for entry in up_copies[at]:
                up_copy(*entry).start()

    up_stage(0)
    lax.fori_loop(1, 3, send_one, 0)

    loads[2].wait()
    loads[3].wait()

    def rs_copy(b):
        return pltpu.make_async_remote_copy(
            src_ref=rs_send.at[b], dst_ref=rs_recv.at[b],
            send_sem=rs_send_sem.at[b], recv_sem=rs_recv_sem.at[b],
            device_id={"ba": lax.rem(mb + b + 1, m)}, device_id_type=MESH,
        )

    def base(b, _):
        cols = pl.ds(pl.multiple_of(lax.rem(mb + b + 1, m) * kv, LANES), kv)
        rs_send[b, :, :kv] = jnp.dot(tok[...], kw[:, cols], preferred_element_type=F32)
        rs_send[b, :, kv:] = jnp.dot(tok[...], vw[:, cols], preferred_element_type=F32)

        @pl.when(b < m - 1)
        def _():
            rs_copy(b).start()

        return 0

    lax.fori_loop(0, m // 2, base, 0)
    up_stage(1)
    lax.fori_loop(3, 5, send_one, 0)
    lax.fori_loop(m // 2, m, base, 0)
    recv[0] = fill(0)
    up_stage(2)
    lax.fori_loop(5, n, send_one, 0)
    loads[4].wait()

    def add_part(b, _):
        rs_copy(b).wait_recv()
        rs_send[m - 1] += rs_recv[b]
        return 0

    width = resident * twice_rank
    slot_of_row = lax.broadcasted_iota(jnp.int32, (chunk, width), 0)
    column = lax.broadcasted_iota(jnp.int32, (chunk, width), 1)
    adapter_of_row = lax.rem(slot_of_row, quads) * groups + slot_of_row // stride
    own = adapter_of_row == column // twice_rank
    for_key = lax.rem(column, twice_rank) < rank

    def part_copy(b, i):
        return pltpu.make_async_remote_copy(
            src_ref=rank_part.at[i], dst_ref=rank_in.at[b, i],
            send_sem=p_send_sem.at[b, i], recv_sem=p_recv_sem.at[b, i],
            device_id={"ba": lax.rem(mb + b + 1, m)}, device_id_type=MESH,
        )

    def ret_copy(i):
        return pltpu.make_async_remote_copy(
            src_ref=ret_send.at[i], dst_ref=ret_recv.at[i],
            send_sem=r_send_sem.at[i], recv_sem=r_recv_sem.at[i],
            device_id={"aa": peer(i)}, device_id_type=MESH,
        )

    def partial(i):
        @pl.when(i > 0)
        def _():
            dispatch(i).wait_recv()

        wide = lax.dot_general(
            recv[i], down[...], (((1,), (1,)), ((), ())), preferred_element_type=F32
        )
        wide = jnp.where(own, wide, 0.0)
        total = wide[:, :LANES]
        for q in range(1, width // LANES):
            total = total + wide[:, q * LANES:(q + 1) * LANES]
        packed = total[:stride]
        for g in range(1, groups):
            packed = packed + total[g * stride:(g + 1) * stride]
        rank_part[i] = packed
        for b in range(m - 1):
            part_copy(b, i).start()

    def finish(i):
        total = rank_part[i]
        for b in range(m - 1):
            part_copy(b, i).wait_recv()
            total = total + rank_in[b, i]

        @pl.when(i == 0)
        def _():
            ret_recv[i] = total

        @pl.when(i > 0)
        def _():
            ret_send[i] = total
            ret_copy(i).start()

    def final(i):
        @pl.when(i > 0)
        def _():
            ret_copy(i).wait_recv()

        tall = jnp.concatenate([ret_recv[i]] * groups, axis=0)
        spread = jnp.where(own, jnp.concatenate([tall] * (width // LANES), axis=1), 0.0)
        key_hi, key_lo = split_two(jnp.where(for_key, spread, 0.0))
        value_hi, value_lo = split_two(jnp.where(for_key, 0.0, spread))
        bank = peer(i)
        up = up_all[bank]
        pieces = jnp.concatenate([key_hi, key_lo, value_hi, value_lo], axis=0)
        out = jnp.dot(pieces, up, preferred_element_type=F32)
        change = jnp.concatenate(
            [out[:chunk] + out[chunk:2 * chunk], out[2 * chunk:3 * chunk] + out[3 * chunk:]], axis=1
        )
        hi, lo = split_two(change)
        place = lax.broadcasted_iota(jnp.int32, (rows, chunk), 1) + bank * chunk
        pick = jnp.where(place == slot_col, 1.0, 0.0).astype(BF16)
        acc[...] += jnp.dot(pick, hi, preferred_element_type=F32) + jnp.dot(
            pick, lo, preferred_element_type=F32
        )

    def step(t, _):
        @pl.when((t >= 1) & (t < n + 1))
        def _():
            finish(t - 1)

        @pl.when(t == 2)
        def _():
            for at in range(3, len(up_copies) + 1):
                up_stage(at)
            lax.fori_loop(0, m - 1, add_part, 0)
            acc[...] = rs_send[m - 1]

        @pl.when(t >= 2)
        def _():
            final(t - 2)

        @pl.when(t < n)
        def _():
            partial(t)

        return 0

    lax.fori_loop(0, n + 2, step, 0)

    for stage in up_copies:
        for entry in stage:
            up_copy(*entry).wait_send()

    def drain(i, _):
        dispatch(i).wait_send()
        ret_copy(i).wait_send()
        return 0

    lax.fori_loop(1, n, drain, 0)

    def drain_parts(i, _):
        for b in range(m - 1):
            part_copy(b, i).wait_send()
        return 0

    lax.fori_loop(0, n, drain_parts, 0)
    for b in range(m - 1):
        rs_copy(b).wait_send()


def xor_bit(x, b):
    return x + b - 2 * b * lax.rem(x // b, 2)


def bits_of(count):
    found = []
    bit = count // 2
    while bit:
        found.append(bit)
        bit //= 2
    return found


def low_bit(mask):
    return mask & -mask


def packed_kernel(
    n, m, direct, shared, near_rows, stride, resident, twice_rank,
    idx_hbm, tok_hbm, kw_hbm, vw_hbm, down_hbm, up_hbm,
    out, flag_hbm,
    idx_mine, idx_all, mine, tri, tok, kw, vw, down, up_all, shared_out, outgoing, recv,
    rs_send, rs_recv, acc, flag, rank_part, rank_in, direct_in, ret_send, ret_recv,
    load_sem, store_sem, x_send_sem, x_recv_sem, idx_send_sem, idx_recv_sem, up_send_sem, up_recv_sem, v_send_sem, v_recv_sem,
    d_send_sem, d_recv_sem, rs_send_sem, rs_recv_sem, p_send_sem, p_recv_sem, r_send_sem, r_recv_sem,
):
    me = lax.axis_index("aa")
    mb = lax.axis_index("ba")
    rows = tok.shape[0]
    kv = acc.shape[1] // 2
    half = n // 2
    slots = direct + shared
    groups = LANES // twice_rank
    packed = rank_part.shape[1]
    rank = twice_rank // 2
    width = resident * twice_rank
    bits = bits_of(n)
    ba_bits = bits_of(m)[::-1]
    count = jnp.int32

    barrier = pltpu.get_barrier_semaphore()

    loads = [
        pltpu.make_async_copy(idx_hbm, idx_mine, load_sem.at[0]),
        pltpu.make_async_copy(
            up_hbm.at[:, pl.ds(pl.multiple_of(mb * kv, LANES), kv)], up_all.at[0], load_sem.at[1]
        ),
        pltpu.make_async_copy(tok_hbm, tok, load_sem.at[2]),
        pltpu.make_async_copy(kw_hbm, kw, load_sem.at[3]),
        pltpu.make_async_copy(vw_hbm, vw, load_sem.at[4]),
        pltpu.make_async_copy(down_hbm, down, load_sem.at[5]),
    ]
    for at in (0, 2, 1, 3, 4, 5):
        loads[at].start()

    def partner(mask):
        other = me
        for b in bits:
            other = jnp.where(lax.rem(mask // b, 2) == 1, xor_bit(other, b), other)
        return other

    def greet_aa(i, _):
        pl.semaphore_signal(barrier, inc=1, device_id={"aa": lax.rem(me + i, n)}, device_id_type=MESH)
        return 0

    def greet_ba(i, _):
        other = lax.rem(mb + i, m)
        pl.semaphore_signal(barrier, inc=1, device_id={"ba": other}, device_id_type=MESH)
        there = {"aa": partner(half + 1), "ba": other}
        pl.semaphore_signal(barrier, inc=1, device_id=there, device_id_type=MESH)
        return 0

    lax.fori_loop(1, n, greet_aa, 0)
    lax.fori_loop(1, m, greet_ba, 0)

    def chosen(masks, t):
        return sum([jnp.where(t == at, mask, 0) for at, mask in enumerate(masks)], jnp.int32(0))

    def idx_copy(mask, source):
        return pltpu.make_async_remote_copy(
            src_ref=idx_mine, dst_ref=idx_all.at[source],
            send_sem=idx_send_sem.at[mask], recv_sem=idx_recv_sem.at[mask],
            device_id={"aa": partner(mask)}, device_id_type=MESH,
        )

    side = half // 2
    inner = lax.rem(me // half + me // side, 2) == 1
    outer = jnp.logical_not(inner)
    across = half + side

    def up_copy(at, source, target, mask):
        return pltpu.make_async_remote_copy(
            src_ref=up_all.at[source], dst_ref=up_all.at[target],
            send_sem=up_send_sem.at[at], recv_sem=up_recv_sem.at[target],
            device_id={"aa": partner(mask)}, device_id_type=MESH,
        )

    own_across = (0, 0, across, across)
    own_side = (1, 0, side, side)
    own_pair = (2, 0, 1, 1)
    pair_copies = {q: (3 + q // side, q, q + 1, 1) for q in (side, half, across)}
    line_copies = {side: (7, side, half, across), across: (8, across, half, side), half: (9, half, across, side)}

    def up_arrived(target):
        up_copy(0, 0, target, target).wait_recv()

    def shared_copy(at, source, target, mask):
        return pltpu.make_async_remote_copy(
            src_ref=source, dst_ref=recv.at[target, pl.ds(direct, shared)],
            send_sem=v_send_sem.at[at], recv_sem=v_recv_sem.at[target],
            device_id={"aa": partner(mask)}, device_id_type=MESH,
        )

    nearest = jnp.where(inner, across, half)

    def shared_first():
        return shared_copy(0, shared_out, nearest, nearest)

    def shared_line(q):
        return shared_copy(1 + (q == half), recv.at[q, pl.ds(direct, shared)], across + half - q, side)

    def shared_pair(q):
        return shared_copy(3 + (q == half), recv.at[q, pl.ds(direct, shared)], q + 1, 1)

    def shared_arrived(q):
        shared_copy(0, shared_out, q, q).wait_recv()

    def row_copy(mask, height):
        return pltpu.make_async_remote_copy(
            src_ref=outgoing.at[mask, pl.ds(0, height)], dst_ref=recv.at[mask, pl.ds(0, height)],
            send_sem=d_send_sem.at[mask], recv_sem=d_recv_sem.at[mask],
            device_id={"aa": partner(mask)}, device_id_type=MESH,
        )

    earlier = lax.broadcasted_iota(count, (rows, rows), 0)
    later = lax.broadcasted_iota(count, (rows, rows), 1)
    tri[...] = jnp.where(earlier < later, 1.0, 0.0).astype(BF16)
    loads[0].wait()
    row = idx_mine[...]
    bank_row = row // resident
    tall = max(16, n)
    match = lax.broadcasted_iota(count, (tall, rows), 0) == bank_row
    ranks = jnp.dot(jnp.where(match, 1.0, 0.0).astype(BF16), tri[...], preferred_element_type=F32)
    rank_row = jnp.sum(jnp.where(match, ranks, 0.0), axis=0, keepdims=True).astype(count)
    far_row = (bank_row // half) != (me // half)
    over_row = jnp.where(far_row & (rank_row >= direct), 1.0, 0.0)
    over_rank = jnp.dot(
        jnp.broadcast_to(over_row, (tall, rows)).astype(BF16), tri[...], preferred_element_type=F32
    )[:1].astype(count)
    slot_row = jnp.where(over_row > 0.5, direct + over_rank, rank_row)
    code_row = bank_row * stride + slot_row
    shared_row = jnp.where(over_row > 0.5, over_rank, -1)

    def gathered(wanted, at):
        pick = jnp.where(wanted == at, 1.0, 0.0).astype(BF16)
        return jnp.dot(pick, tok[...], preferred_element_type=F32).astype(BF16)

    def fill(bank, height):
        return gathered(lax.broadcasted_iota(count, (height, rows), 0) + bank * stride, code_row)

    loads[2].wait()
    shared_out[...] = gathered(lax.broadcasted_iota(count, (shared, rows), 0), shared_row)
    pl.semaphore_wait(barrier, n - 1 + 2 * (m - 1))

    def send_idx(mask, _):
        idx_copy(mask, me).start()
        return 0

    lax.fori_loop(1, n, send_idx, 0)
    shared_first().start()
    loads[1].wait()

    @pl.when(inner)
    def _():
        up_copy(*own_across).start()

    up_copy(*own_side).start()

    def send_near(mask, _):
        outgoing[mask] = fill(partner(mask), near_rows)
        row_copy(mask, near_rows).start()
        return 0

    def send_far(mask, _):
        outgoing[mask, pl.ds(0, direct)] = fill(partner(mask), direct)
        row_copy(mask, direct).start()
        return 0

    lax.fori_loop(side, side + 1, send_near, 0)
    lax.fori_loop(1, 2, send_near, 0)

    def rs_copy(q):
        hop = low_bit(q)
        return pltpu.make_async_remote_copy(
            src_ref=rs_send.at[q], dst_ref=rs_recv.at[q],
            send_sem=rs_send_sem.at[q], recv_sem=rs_recv_sem.at[q],
            device_id={"ba": xor_bit(mb, hop)}, device_id_type=MESH,
        )

    loads[3].wait()
    loads[4].wait()
    base_order = sorted(range(1, m), key=lambda q: (low_bit(q), q)) + [0]

    def base(t, _):
        q = chosen(base_order, t)
        block = mb
        for b in ba_bits:
            block = jnp.where(lax.rem(q // b, 2) == 1, xor_bit(block, b), block)
        cols = pl.ds(pl.multiple_of(block * kv, LANES), kv)
        rs_send[q, :, :kv] = jnp.dot(tok[...], kw[:, cols], preferred_element_type=F32)
        rs_send[q, :, kv:] = jnp.dot(tok[...], vw[:, cols], preferred_element_type=F32)
        for at, q_now in enumerate(base_order):
            if q_now:
                @pl.when(t == at)
                def _():
                    for b in ba_bits:
                        if b < low_bit(q_now):
                            rs_copy(q_now + b).wait_recv()
                            rs_send[q_now] += rs_recv[q_now + b]
                    rs_copy(q_now).start()

        return 0

    lax.fori_loop(0, m, base, 0)

    idx_all[me] = row
    for_self = fill(me, near_rows)
    recv[0, pl.ds(0, near_rows)] = for_self
    for mask in range(half):
        recv[mask, pl.ds(near_rows, slots - near_rows)] = jnp.zeros((slots - near_rows, tok.shape[1]), BF16)

    def wait_idx(mask, _):
        idx_copy(mask, partner(mask)).wait_recv()
        return 0

    lax.fori_loop(1, n, wait_idx, 0)
    everyone = jnp.concatenate([idx_all[s] for s in range(n)], axis=0)
    banks = everyone // resident
    matches = [banks == b for b in range(n)]
    stacked = jnp.concatenate([jnp.where(hit, 1.0, 0.0) for hit in matches], axis=0)
    all_ranks = jnp.dot(stacked.astype(BF16), tri[...], preferred_element_type=F32)
    place = jnp.zeros((n, rows), F32)
    for b in range(n):
        place = place + jnp.where(matches[b], all_ranks[b * n:(b + 1) * n], 0.0)
    place = place.astype(count)
    far_all = (banks // half) != (lax.broadcasted_iota(count, (n, rows), 0) // half)
    over_all = jnp.where(far_all & (place >= direct), 1.0, 0.0)
    padded = jnp.concatenate([over_all] * (tall // n), axis=0)
    over_ranks = jnp.dot(padded.astype(BF16), tri[...], preferred_element_type=F32)[:n].astype(count)
    place = jnp.where(over_all > 0.5, direct + over_ranks, place)
    excess = jnp.where(place >= jnp.where(far_all, slots, near_rows), 1, 0)
    flag[0] = jnp.max(excess)
    flag_copy = pltpu.make_async_copy(flag, flag_hbm, store_sem.at[0])
    flag_copy.start()
    to_me = jnp.where(banks == me, place, -1)
    for s in range(n):
        mine[s] = to_me[s:s + 1]
    code_col = jnp.sum(jnp.where(earlier == later, code_row, 0), axis=1, keepdims=True)

    lane = lax.broadcasted_iota(count, (packed, LANES), 1) // twice_rank
    column = lax.broadcasted_iota(count, (slots, width), 1)
    for_key = lax.rem(column, twice_rank) < rank

    def folded(x):
        total = x
        for g in range(1, groups):
            total = total + pltpu.roll(x, g * twice_rank, axis=1)
        return total

    def owned(wanted, at, ids):
        local = jnp.sum(jnp.where(wanted == at, lax.rem(ids, resident), 0), axis=1, keepdims=True)
        return local == column // twice_rank

    def part_copy(b, mask):
        return pltpu.make_async_remote_copy(
            src_ref=rank_part.at[mask], dst_ref=rank_in.at[b, mask],
            send_sem=p_send_sem.at[b, mask], recv_sem=p_recv_sem.at[b, mask],
            device_id={"ba": lax.rem(mb + b + 1, m)}, device_id_type=MESH,
        )

    def direct_copy(b):
        return pltpu.make_async_remote_copy(
            src_ref=rank_part.at[half + 1], dst_ref=direct_in.at[b],
            send_sem=x_send_sem.at[b], recv_sem=x_recv_sem.at[b],
            device_id={"aa": partner(half + 1), "ba": lax.rem(mb + b, m)}, device_id_type=MESH,
        )

    def goes_direct(mask):
        return mask == half + 1

    def ret_copy(mask):
        return pltpu.make_async_remote_copy(
            src_ref=ret_send.at[mask], dst_ref=ret_recv.at[mask],
            send_sem=r_send_sem.at[mask], recv_sem=r_recv_sem.at[mask],
            device_id={"aa": partner(mask)}, device_id_type=MESH,
        )

    def partial(mask):
        @pl.when((mask > 0) & (mask < half))
        def _():
            row_copy(mask, near_rows).wait_recv()

        @pl.when(mask >= half)
        def _():
            row_copy(mask, direct).wait_recv()

        source = partner(mask)
        wide = lax.dot_general(
            recv[mask], down[...], (((1,), (1,)), ((), ())), preferred_element_type=F32
        )
        own = owned(lax.broadcasted_iota(count, (slots, rows), 0), mine[source], idx_all[source])
        wide = jnp.where(own, wide, 0.0)
        total = wide[:, :LANES]
        for q in range(1, width // LANES):
            total = total + wide[:, q * LANES:(q + 1) * LANES]
        total = folded(total)
        if groups * packed > slots:
            total = jnp.concatenate([total, jnp.zeros((groups * packed - slots, LANES), F32)], axis=0)
        together = total[:packed]
        for g in range(1, groups):
            together = jnp.where(lane == g, total[g * packed:(g + 1) * packed], together)
        rank_part[mask] = together

        @pl.when(jnp.logical_not(goes_direct(mask) & outer))
        def _():
            for b in range(m - 1):
                part_copy(b, mask).start()

        @pl.when(goes_direct(mask) & outer)
        def _():
            for b in range(m):
                direct_copy(b).start()

    def finish(mask):
        total = rank_part[mask]
        for b in range(m - 1):
            part_copy(b, mask).wait_recv()
            total = total + rank_in[b, mask]

        @pl.when(mask == 0)
        def _():
            ret_recv[mask] = total

        @pl.when(mask > 0)
        def _():
            ret_send[mask] = total
            ret_copy(mask).start()

    def final(mask):
        @pl.when((mask > 0) & jnp.logical_not(goes_direct(mask) & inner))
        def _():
            ret_copy(mask).wait_recv()

        @pl.when(goes_direct(mask) & inner)
        def _():
            total = jnp.zeros((packed, LANES), F32)
            for b in range(m):
                direct_copy(b).wait_recv()
                total = total + direct_in[b]
            ret_recv[half + 1] = total

        bank = partner(mask)
        together = ret_recv[mask]
        tall_ranks = jnp.concatenate(
            [folded(jnp.where(lane == g, together, 0.0)) for g in range(groups)], axis=0
        )[:slots]
        own = owned(lax.broadcasted_iota(count, (slots, rows), 0) + bank * stride, code_row, row)
        spread = jnp.where(own, jnp.concatenate([tall_ranks] * (width // LANES), axis=1), 0.0)
        key_hi, key_lo = split_two(jnp.where(for_key, spread, 0.0))
        value_hi, value_lo = split_two(jnp.where(for_key, 0.0, spread))
        pieces = jnp.concatenate([key_hi, key_lo, value_hi, value_lo], axis=0)
        out = jnp.dot(pieces, up_all[mask], preferred_element_type=F32)
        change = jnp.concatenate(
            [out[:slots] + out[slots:2 * slots], out[2 * slots:3 * slots] + out[3 * slots:]], axis=1
        )
        hi, lo = split_two(change)
        pick = jnp.where(
            lax.broadcasted_iota(count, (rows, slots), 1) + bank * stride == code_col, 1.0, 0.0
        ).astype(BF16)
        acc[...] += jnp.dot(pick, hi, preferred_element_type=F32) + jnp.dot(
            pick, lo, preferred_element_type=F32
        )

    loads[5].wait()

    def line_up(q):
        up_arrived(q)

        @pl.when(inner)
        def _():
            up_copy(*line_copies[q]).start()

    def pair_up(q):
        up_copy(*pair_copies[q]).start()

    def pair_shared(q):
        shared_arrived(q)
        shared_pair(q).start()

    def init():
        for b in ba_bits:
            rs_copy(b).wait_recv()
            rs_send[0] += rs_recv[b]
        acc[...] = rs_send[0]

    two, three, four, five, six, seven = side, side + 1, half, half + 1, across, across + 1
    inner_turns = [
        (0, 0), (0, 1),
        (0, two), (0, four), (0, five), (1, 0), (2, 0), (1, 1), (1, two), (1, four), (1, five), (3, four),
        (0, three), (0, six), (1, three), (0, seven), (1, six), (2, 1), (1, seven), (3, five), (2, two), (2, three),
        (2, six), (2, seven), (2, four), (2, five),
    ]
    outer_turns = [
        (0, 0), (0, 1),
        (0, two), (1, 0), (2, 0), (1, 1), (1, two), (0, three), (0, six), (1, three), (0, seven), (1, six),
        (2, 1), (1, seven), (2, two), (2, four), (0, four), (2, three), (1, four), (2, five), (2, six), (0, five),
        (2, seven), (4, 0), (4, 0), (4, 0),
    ]
    opening = 2

    def turn(t, _):
        kind = jnp.where(inner, chosen([k for k, _ in inner_turns], t), chosen([k for k, _ in outer_turns], t))
        mask = jnp.where(inner, chosen([q for _, q in inner_turns], t), chosen([q for _, q in outer_turns], t))

        @pl.when((kind == 1) & (mask == 0) & outer)
        def _():
            pair_shared(across)
            pair_shared(half)

        for q in (half + 1, across + 1):
            @pl.when((kind == 0) & (mask == q))
            def _():
                shared_arrived(q)

        @pl.when((kind == 1) & (mask == jnp.where(inner, half, side + 1)))
        def _():
            line_up(half)
            pair_up(half)

        @pl.when((kind == 2) & (mask == 1) & outer)
        def _():
            line_up(across)
            pair_up(across)

        @pl.when((kind == 2) & (mask == 0))
        def _():
            init()

        for q in range(1, n, 2):
            @pl.when((kind == 2) & (mask == q))
            def _():
                up_arrived(q)

        @pl.when(kind == 0)
        def _():
            partial(mask)

        @pl.when(kind == 1)
        def _():
            finish(mask)

        @pl.when(kind == 2)
        def _():
            final(mask)

        @pl.when(kind == 3)
        def _():
            send_far(mask, 0)

        return 0

    @pl.when(inner)
    def _():
        for q in (half, across):
            shared_arrived(q)
            shared_line(q).start()
            shared_pair(q).start()

    line_up(side)
    lax.fori_loop(0, 2, lambda t, _: send_far(nearest + t, 0), 0)
    lax.fori_loop(side + 1, side + 2, send_near, 0)

    @pl.when(outer)
    def _():
        lax.fori_loop(across, across + 2, send_far, 0)

    up_copy(*own_pair).start()
    pair_up(side)
    lax.fori_loop(0, opening, turn, 0)

    @pl.when(inner)
    def _():
        line_up(across)
        pair_up(across)

    lax.fori_loop(opening, len(inner_turns), turn, 0)
    out[...] = acc[...].astype(BF16)

    shared_first().wait_send()
    for copy in (own_side, own_pair, *pair_copies.values()):
        up_copy(*copy).wait_send()
    for q in (half, across):
        shared_pair(q).wait_send()

    @pl.when(inner)
    def _():
        for copy in (own_across, *line_copies.values()):
            up_copy(*copy).wait_send()
        for q in (half, across):
            shared_line(q).wait_send()

    def drain(mask, _):
        idx_copy(mask, me).wait_send()

        @pl.when(jnp.logical_not(goes_direct(mask) & outer))
        def _():
            ret_copy(mask).wait_send()

        @pl.when(mask < half)
        def _():
            row_copy(mask, near_rows).wait_send()

        @pl.when(mask >= half)
        def _():
            row_copy(mask, direct).wait_send()

        return 0

    lax.fori_loop(1, n, drain, 0)

    def drain_parts(mask, _):
        @pl.when(jnp.logical_not(goes_direct(mask) & outer))
        def _():
            for b in range(m - 1):
                part_copy(b, mask).wait_send()

        return 0

    lax.fori_loop(0, n, drain_parts, 0)

    @pl.when(outer)
    def _():
        for b in range(m):
            direct_copy(b).wait_send()

    for q in range(1, m):
        rs_copy(q).wait_send()
    flag_copy.wait()


def packed_call(n, m, cap, idx, tokens, key_weight, value_weight, down_flat, up_flat, resident):
    rows, width = tokens.shape
    flat = down_flat.shape[0]
    twice_rank = flat // resident
    kv_width = key_weight.shape[1]
    kv = kv_width // m
    direct = rows // n
    shared = 5 * direct // 8
    near_rows = 3 * direct // 2
    slots = direct + shared
    stride = resident * cap
    packed = stride * twice_rank // LANES
    dma = pltpu.SemaphoreType.DMA
    return pl.pallas_call(
        functools.partial(packed_kernel, n, m, direct, shared, near_rows, stride, resident, twice_rank),
        out_shape=[
            jax.ShapeDtypeStruct((rows, 2 * kv), BF16),
            jax.ShapeDtypeStruct((1,), jnp.int32),
        ],
        in_specs=[pl.BlockSpec(memory_space=pltpu.HBM)] * 6,
        out_specs=[pl.BlockSpec(memory_space=pltpu.VMEM), pl.BlockSpec(memory_space=pltpu.HBM)],
        scratch_shapes=[
            pltpu.VMEM((1, rows), jnp.int32),
            pltpu.VMEM((n, 1, rows), jnp.int32),
            pltpu.VMEM((n, 1, rows), jnp.int32),
            pltpu.VMEM((rows, rows), BF16),
            pltpu.VMEM((rows, width), BF16),
            pltpu.VMEM((width, kv_width), BF16),
            pltpu.VMEM((width, kv_width), BF16),
            pltpu.VMEM((flat, width), BF16),
            pltpu.VMEM((n, flat, kv), BF16),
            pltpu.VMEM((shared, width), BF16),
            pltpu.VMEM((n, near_rows, width), BF16),
            pltpu.VMEM((n, slots, width), BF16),
            pltpu.VMEM((m, rows, 2 * kv), F32),
            pltpu.VMEM((m, rows, 2 * kv), F32),
            pltpu.VMEM((rows, 2 * kv), F32),
            pltpu.SMEM((1,), jnp.int32),
            pltpu.VMEM((n, packed, LANES), F32),
            pltpu.VMEM((m - 1, n, packed, LANES), F32),
            pltpu.VMEM((m, packed, LANES), F32),
            pltpu.VMEM((n, packed, LANES), F32),
            pltpu.VMEM((n, packed, LANES), F32),
            dma((6,)), dma((1,)), dma((m,)), dma((m,)),
            dma((n,)), dma((n,)), dma((10,)), dma((n,)), dma((5,)), dma((n,)),
            dma((n,)), dma((n,)),
            dma((m,)), dma((m,)),
            dma((m - 1, n)), dma((m - 1, n)),
            dma((n,)), dma((n,)),
        ],
        compiler_params=pltpu.CompilerParams(
            collective_id=1, has_side_effects=True, vmem_limit_bytes=63 * 1024 * 1024
        ),
    )(idx, tokens, key_weight, value_weight, down_flat, up_flat)


def on_device(n, m, tokens, request_adapter_index, key_weight, value_weight, down_weight, up_weight):
    rows, width = tokens.shape
    resident, twice_rank, _ = down_weight.shape
    kv_width = key_weight.shape[1]
    kv = kv_width // m
    cap = max(2, 2 * rows // (resident * n))
    chunk = resident * cap
    packed = chunk * twice_rank // LANES
    flat = resident * twice_rank
    operands = (
        request_adapter_index.reshape(1, rows),
        tokens,
        key_weight,
        value_weight,
        down_weight.reshape(flat, width),
        up_weight.reshape(flat, kv_width),
    )

    def any_load():
        dma = pltpu.SemaphoreType.DMA
        total = pl.pallas_call(
            functools.partial(kernel, n, m, cap, resident, twice_rank),
            out_shape=jax.ShapeDtypeStruct((rows, 2 * kv), F32),
            in_specs=[pl.BlockSpec(memory_space=pltpu.VMEM)] + [pl.BlockSpec(memory_space=pltpu.HBM)] * 5,
            out_specs=pl.BlockSpec(memory_space=pltpu.VMEM),
            scratch_shapes=[
                pltpu.VMEM((rows, width), BF16),
                pltpu.VMEM((width, kv_width), BF16),
                pltpu.VMEM((width, kv_width), BF16),
                pltpu.VMEM((flat, width), BF16),
                pltpu.VMEM((n, flat, kv), BF16),
                pltpu.VMEM((n, chunk, width), BF16),
                pltpu.VMEM((n, chunk, width), BF16),
                pltpu.VMEM((m, rows, 2 * kv), F32),
                pltpu.VMEM((m - 1, rows, 2 * kv), F32),
                pltpu.VMEM((n, packed, LANES), F32),
                pltpu.VMEM((m - 1, n, packed, LANES), F32),
                pltpu.VMEM((n, packed, LANES), F32),
                pltpu.VMEM((n, packed, LANES), F32),
                dma((5,)),
                dma((n,)), dma((n,)), dma((n,)), dma((n,)),
                dma((m,)), dma((m,)),
                dma((m - 1, n)), dma((m - 1, n)),
                dma((n,)), dma((n,)),
            ],
            compiler_params=pltpu.CompilerParams(
                collective_id=0, has_side_effects=True, vmem_limit_bytes=56 * 1024 * 1024
            ),
        )(
            *operands,
        )
        return total.astype(BF16)

    if n // 2 != 4 or rows % (64 * n) or 13 * rows // (8 * n) >= chunk:
        both = any_load()
    else:
        both, flag = packed_call(n, m, cap, *operands, resident)
        both = lax.cond(flag.reshape(()) > 0, any_load, lambda: both)
    return both[:, :kv], both[:, kv:]


def solution(mesh):
    return jax.shard_map(
        functools.partial(on_device, mesh.shape["aa"], mesh.shape["ba"]),
        mesh=mesh,
        in_specs=(
            P("aa", "ba"),
            P("aa", None),
            P("ba", None),
            P("ba", None),
            P("aa", None, "ba"),
            P("aa", None, None, None),
        ),
        out_specs=(P("aa", "ba"), P("aa", "ba")),
        check_vma=False,
    )
```

```python
import functools

import jax
import jax.numpy as jnp
from jax import lax
from jax.experimental import pallas as pl
from jax.experimental.pallas import tpu as pltpu
from jax.sharding import PartitionSpec as P

MESH = pl.DeviceIdType.MESH
LANES = 128
BF16 = jnp.bfloat16
F32 = jnp.float32


def split_two(x):
    hi = x.astype(BF16)
    return hi, (x - hi.astype(F32)).astype(BF16)


def kernel(
    n, m, cap, resident, twice_rank,
    idx_row, tok_hbm, kw_hbm, vw_hbm, down_hbm, up_hbm,
    acc,
    tok, kw, vw, down, up_all, outgoing, recv, rs_send, rs_recv,
    rank_part, rank_in, ret_send, ret_recv,
    load_sem, up_send_sem, up_recv_sem, d_send_sem, d_recv_sem,
    rs_send_sem, rs_recv_sem, p_send_sem, p_recv_sem, r_send_sem, r_recv_sem,
):
    me = lax.axis_index("aa")
    mb = lax.axis_index("ba")
    rows = tok.shape[0]
    kv = acc.shape[1] // 2
    groups = LANES // twice_rank
    quads = resident // groups
    stride = cap * quads
    chunk = resident * cap
    rank = twice_rank // 2

    loads = [
        pltpu.make_async_copy(tok_hbm, tok, load_sem.at[0]),
        pltpu.make_async_copy(
            up_hbm.at[:, pl.ds(pl.multiple_of(mb * kv, LANES), kv)], up_all.at[me], load_sem.at[1]
        ),
        pltpu.make_async_copy(kw_hbm, kw, load_sem.at[2]),
        pltpu.make_async_copy(vw_hbm, vw, load_sem.at[3]),
        pltpu.make_async_copy(down_hbm, down, load_sem.at[4]),
    ]
    for c in loads:
        c.start()

    barrier = pltpu.get_barrier_semaphore()

    def greet_aa(i, _):
        pl.semaphore_signal(barrier, inc=1, device_id={"aa": lax.rem(me + i, n)}, device_id_type=MESH)
        return 0

    def greet_ba(i, _):
        pl.semaphore_signal(barrier, inc=1, device_id={"ba": lax.rem(mb + i, m)}, device_id_type=MESH)
        return 0

    lax.fori_loop(1, n, greet_aa, 0)
    lax.fori_loop(1, m, greet_ba, 0)

    def slot(a, earlier):
        local = lax.rem(a, resident)
        return (a // resident) * chunk + lax.rem(local, groups) * stride + earlier * quads + local // groups

    row = idx_row[...]
    down_pos = lax.broadcasted_iota(jnp.int32, (rows, rows), 0)
    lane_pos = lax.broadcasted_iota(jnp.int32, (rows, rows), 1)
    col = jnp.sum(jnp.where(down_pos == lane_pos, row, 0), axis=1, keepdims=True)
    same = col == row
    slot_col = slot(col, jnp.sum(jnp.where(same & (lane_pos < down_pos), 1, 0), axis=1, keepdims=True))
    slot_row = slot(row, jnp.sum(jnp.where(same & (down_pos < lane_pos), 1, 0), axis=0, keepdims=True))

    def flip(x, b):
        return x + b - 2 * b * lax.rem(x // b, 2)

    bits = []
    bit = n // 2
    while bit:
        bits.append(bit)
        bit //= 2

    far = list(range(n // 2, n))
    near = list(range(n // 4, n // 2))
    order = [0]
    while far:
        if near:
            order.append(near.pop(0))
        order.append(far.pop(0))
    order += near + [d for d in range(n // 4 - 1, 0, -1)]

    def peer(i):
        mask = sum([jnp.where(i == at, order[at], 0) for at in range(1, n)], jnp.int32(0))
        other = me
        for b in bits:
            other = jnp.where(lax.rem(mask // b, 2) == 1, flip(other, b), other)
        return other

    def dispatch(i):
        return pltpu.make_async_remote_copy(
            src_ref=outgoing.at[i], dst_ref=recv.at[i],
            send_sem=d_send_sem.at[i], recv_sem=d_recv_sem.at[i],
            device_id={"aa": peer(i)}, device_id_type=MESH,
        )

    def fill(i):
        wanted = lax.broadcasted_iota(jnp.int32, (chunk, rows), 0) + peer(i) * chunk
        pick = jnp.where(wanted == slot_row, 1.0, 0.0).astype(BF16)
        return jnp.dot(pick, tok[...], preferred_element_type=F32).astype(BF16)

    up_copies = []
    held = [()]
    number = 0
    for b in bits:
        stage = []
        for path in held:
            block = me
            for q in path:
                block = flip(block, q)
            stage.append((block, flip(me, b), number))
            number += 1
        up_copies.append(stage)
        held = held + [path + (b,) for path in held]

    def up_copy(block, partner, at):
        return pltpu.make_async_remote_copy(
            src_ref=up_all.at[block], dst_ref=up_all.at[block],
            send_sem=up_send_sem.at[at], recv_sem=up_recv_sem.at[at],
            device_id={"aa": partner}, device_id_type=MESH,
        )

    pl.semaphore_wait(barrier, n + m - 2)
    loads[1].wait()
    loads[0].wait()

    def send_one(i, _):
        outgoing[i] = fill(i)
        dispatch(i).start()
        return 0

    def up_stage(at):
        if at > 0:
            for entry in up_copies[at - 1]:
                up_copy(*entry).wait_recv()
        if at < len(up_copies):
            for entry in up_copies[at]:
                up_copy(*entry).start()

    up_stage(0)
    lax.fori_loop(1, 3, send_one, 0)

    loads[2].wait()
    loads[3].wait()

    def rs_copy(b):
        return pltpu.make_async_remote_copy(
            src_ref=rs_send.at[b], dst_ref=rs_recv.at[b],
            send_sem=rs_send_sem.at[b], recv_sem=rs_recv_sem.at[b],
            device_id={"ba": lax.rem(mb + b + 1, m)}, device_id_type=MESH,
        )

    def base(b, _):
        cols = pl.ds(pl.multiple_of(lax.rem(mb + b + 1, m) * kv, LANES), kv)
        rs_send[b, :, :kv] = jnp.dot(tok[...], kw[:, cols], preferred_element_type=F32)
        rs_send[b, :, kv:] = jnp.dot(tok[...], vw[:, cols], preferred_element_type=F32)

        @pl.when(b < m - 1)
        def _():
            rs_copy(b).start()

        return 0

    lax.fori_loop(0, m // 2, base, 0)
    up_stage(1)
    lax.fori_loop(3, 5, send_one, 0)
    lax.fori_loop(m // 2, m, base, 0)
    recv[0] = fill(0)
    up_stage(2)
    lax.fori_loop(5, n, send_one, 0)
    loads[4].wait()

    def add_part(b, _):
        rs_copy(b).wait_recv()
        rs_send[m - 1] += rs_recv[b]
        return 0

    width = resident * twice_rank
    slot_of_row = lax.broadcasted_iota(jnp.int32, (chunk, width), 0)
    column = lax.broadcasted_iota(jnp.int32, (chunk, width), 1)
    adapter_of_row = lax.rem(slot_of_row, quads) * groups + slot_of_row // stride
    own = adapter_of_row == column // twice_rank
    for_key = lax.rem(column, twice_rank) < rank

    def part_copy(b, i):
        return pltpu.make_async_remote_copy(
            src_ref=rank_part.at[i], dst_ref=rank_in.at[b, i],
            send_sem=p_send_sem.at[b, i], recv_sem=p_recv_sem.at[b, i],
            device_id={"ba": lax.rem(mb + b + 1, m)}, device_id_type=MESH,
        )

    def ret_copy(i):
        return pltpu.make_async_remote_copy(
            src_ref=ret_send.at[i], dst_ref=ret_recv.at[i],
            send_sem=r_send_sem.at[i], recv_sem=r_recv_sem.at[i],
            device_id={"aa": peer(i)}, device_id_type=MESH,
        )

    def partial(i):
        @pl.when(i > 0)
        def _():
            dispatch(i).wait_recv()

        wide = lax.dot_general(
            recv[i], down[...], (((1,), (1,)), ((), ())), preferred_element_type=F32
        )
        wide = jnp.where(own, wide, 0.0)
        total = wide[:, :LANES]
        for q in range(1, width // LANES):
            total = total + wide[:, q * LANES:(q + 1) * LANES]
        packed = total[:stride]
        for g in range(1, groups):
            packed = packed + total[g * stride:(g + 1) * stride]
        rank_part[i] = packed
        for b in range(m - 1):
            part_copy(b, i).start()

    def finish(i):
        total = rank_part[i]
        for b in range(m - 1):
            part_copy(b, i).wait_recv()
            total = total + rank_in[b, i]

        @pl.when(i == 0)
        def _():
            ret_recv[i] = total

        @pl.when(i > 0)
        def _():
            ret_send[i] = total
            ret_copy(i).start()

    def final(i):
        @pl.when(i > 0)
        def _():
            ret_copy(i).wait_recv()

        tall = jnp.concatenate([ret_recv[i]] * groups, axis=0)
        spread = jnp.where(own, jnp.concatenate([tall] * (width // LANES), axis=1), 0.0)
        key_hi, key_lo = split_two(jnp.where(for_key, spread, 0.0))
        value_hi, value_lo = split_two(jnp.where(for_key, 0.0, spread))
        bank = peer(i)
        up = up_all[bank]
        pieces = jnp.concatenate([key_hi, key_lo, value_hi, value_lo], axis=0)
        out = jnp.dot(pieces, up, preferred_element_type=F32)
        change = jnp.concatenate(
            [out[:chunk] + out[chunk:2 * chunk], out[2 * chunk:3 * chunk] + out[3 * chunk:]], axis=1
        )
        hi, lo = split_two(change)
        place = lax.broadcasted_iota(jnp.int32, (rows, chunk), 1) + bank * chunk
        pick = jnp.where(place == slot_col, 1.0, 0.0).astype(BF16)
        acc[...] += jnp.dot(pick, hi, preferred_element_type=F32) + jnp.dot(
            pick, lo, preferred_element_type=F32
        )

    def step(t, _):
        @pl.when((t >= 1) & (t < n + 1))
        def _():
            finish(t - 1)

        @pl.when(t == 2)
        def _():
            for at in range(3, len(up_copies) + 1):
                up_stage(at)
            lax.fori_loop(0, m - 1, add_part, 0)
            acc[...] = rs_send[m - 1]

        @pl.when(t >= 2)
        def _():
            final(t - 2)

        @pl.when(t < n)
        def _():
            partial(t)

        return 0

    lax.fori_loop(0, n + 2, step, 0)

    for stage in up_copies:
        for entry in stage:
            up_copy(*entry).wait_send()

    def drain(i, _):
        dispatch(i).wait_send()
        ret_copy(i).wait_send()
        return 0

    lax.fori_loop(1, n, drain, 0)

    def drain_parts(i, _):
        for b in range(m - 1):
            part_copy(b, i).wait_send()
        return 0

    lax.fori_loop(0, n, drain_parts, 0)
    for b in range(m - 1):
        rs_copy(b).wait_send()


def xor_bit(x, b):
    return x + b - 2 * b * lax.rem(x // b, 2)


def bits_of(count):
    found = []
    bit = count // 2
    while bit:
        found.append(bit)
        bit //= 2
    return found


def low_bit(mask):
    return mask & -mask


def packed_kernel(
    n, m, direct, shared, near_rows, stride, resident, twice_rank,
    idx_hbm, tok_hbm, kw_hbm, vw_hbm, down_hbm, up_hbm,
    out, flag_hbm,
    idx_mine, idx_all, mine, tri, tok, kw, vw, down, down_t, up_all, shared_out, outgoing, recv,
    rs_send, rs_recv, acc, flag, rank_part, rank_in, direct_in, ret_send, ret_recv,
    load_sem, store_sem, x_send_sem, x_recv_sem, idx_send_sem, idx_recv_sem, up_send_sem, up_recv_sem, v_send_sem, v_recv_sem,
    d_send_sem, d_recv_sem, rs_send_sem, rs_recv_sem, p_send_sem, p_recv_sem, r_send_sem, r_recv_sem,
):
    me = lax.axis_index("aa")
    mb = lax.axis_index("ba")
    rows = tok.shape[0]
    kv = acc.shape[1] // 2
    half = n // 2
    slots = direct + shared
    groups = LANES // twice_rank
    packed = rank_part.shape[1]
    rank = twice_rank // 2
    width = resident * twice_rank
    bits = bits_of(n)
    ba_bits = bits_of(m)[::-1]
    count = jnp.int32

    barrier = pltpu.get_barrier_semaphore()

    loads = [
        pltpu.make_async_copy(idx_hbm, idx_mine, load_sem.at[0]),
        pltpu.make_async_copy(
            up_hbm.at[:, pl.ds(pl.multiple_of(mb * kv, LANES), kv)], up_all.at[0], load_sem.at[1]
        ),
        pltpu.make_async_copy(tok_hbm, tok, load_sem.at[2]),
        pltpu.make_async_copy(kw_hbm, kw, load_sem.at[3]),
        pltpu.make_async_copy(vw_hbm, vw, load_sem.at[4]),
        pltpu.make_async_copy(down_hbm, down, load_sem.at[5]),
    ]
    for at in (0, 2, 1, 3, 4, 5):
        loads[at].start()

    def partner(mask):
        other = me
        for b in bits:
            other = jnp.where(lax.rem(mask // b, 2) == 1, xor_bit(other, b), other)
        return other

    def greet_aa(i, _):
        pl.semaphore_signal(barrier, inc=1, device_id={"aa": lax.rem(me + i, n)}, device_id_type=MESH)
        return 0

    def greet_ba(i, _):
        other = lax.rem(mb + i, m)
        pl.semaphore_signal(barrier, inc=1, device_id={"ba": other}, device_id_type=MESH)
        there = {"aa": partner(half + 1), "ba": other}
        pl.semaphore_signal(barrier, inc=1, device_id=there, device_id_type=MESH)
        return 0

    lax.fori_loop(1, n, greet_aa, 0)
    lax.fori_loop(1, m, greet_ba, 0)

    def chosen(masks, t):
        return sum([jnp.where(t == at, mask, 0) for at, mask in enumerate(masks)], jnp.int32(0))

    def landed(ref, sem):
        pltpu.make_async_copy(ref, ref, sem).wait()

    def idx_copy(mask, source):
        return pltpu.make_async_remote_copy(
            src_ref=idx_mine, dst_ref=idx_all.at[source],
            send_sem=idx_send_sem.at[0], recv_sem=idx_recv_sem.at[0],
            device_id={"aa": partner(mask)}, device_id_type=MESH,
        )

    side = half // 2
    inner = lax.rem(me // half + me // side, 2) == 1
    outer = jnp.logical_not(inner)
    across = half + side

    def up_copy(at, source, target, mask):
        return pltpu.make_async_remote_copy(
            src_ref=up_all.at[source], dst_ref=up_all.at[target],
            send_sem=up_send_sem.at[at], recv_sem=up_recv_sem.at[target],
            device_id={"aa": partner(mask)}, device_id_type=MESH,
        )

    own_across = (0, 0, across, across)
    own_side = (1, 0, side, side)
    own_pair = (2, 0, 1, 1)
    pair_copies = {q: (3 + q // side, q, q + 1, 1) for q in (side, half, across)}
    line_copies = {side: (7, side, half, across), across: (8, across, half, side), half: (9, half, across, side)}

    def up_arrived(target):
        up_copy(0, 0, target, target).wait_recv()

    def shared_copy(at, source, target, mask):
        return pltpu.make_async_remote_copy(
            src_ref=source, dst_ref=recv.at[target, pl.ds(direct, shared)],
            send_sem=v_send_sem.at[at], recv_sem=v_recv_sem.at[target],
            device_id={"aa": partner(mask)}, device_id_type=MESH,
        )

    nearest = jnp.where(inner, across, half)

    def shared_first():
        return shared_copy(0, shared_out, nearest, nearest)

    def shared_line(q):
        return shared_copy(1 + (q == half), recv.at[q, pl.ds(direct, shared)], across + half - q, side)

    def shared_pair(q):
        return shared_copy(3 + (q == half), recv.at[q, pl.ds(direct, shared)], q + 1, 1)

    def shared_arrived(q):
        shared_copy(0, shared_out, q, q).wait_recv()

    def row_copy(mask, height):
        return pltpu.make_async_remote_copy(
            src_ref=outgoing.at[mask, pl.ds(0, height)], dst_ref=recv.at[mask, pl.ds(0, height)],
            send_sem=d_send_sem.at[mask], recv_sem=d_recv_sem.at[mask],
            device_id={"aa": partner(mask)}, device_id_type=MESH,
        )

    earlier = lax.broadcasted_iota(count, (rows, rows), 0)
    later = lax.broadcasted_iota(count, (rows, rows), 1)
    tri[...] = jnp.where(earlier < later, 1.0, 0.0).astype(BF16)
    loads[0].wait()
    row = idx_mine[...]
    bank_row = row // resident
    tall = max(16, n)
    match = lax.broadcasted_iota(count, (tall, rows), 0) == bank_row
    ranks = jnp.dot(jnp.where(match, 1.0, 0.0).astype(BF16), tri[...], preferred_element_type=F32)
    rank_row = jnp.sum(jnp.where(match, ranks, 0.0), axis=0, keepdims=True).astype(count)
    far_row = (bank_row // half) != (me // half)
    over_row = jnp.where(far_row & (rank_row >= direct), 1.0, 0.0)
    over_rank = jnp.dot(
        jnp.broadcast_to(over_row, (tall, rows)).astype(BF16), tri[...], preferred_element_type=F32
    )[:1].astype(count)
    slot_row = jnp.where(over_row > 0.5, direct + over_rank, rank_row)
    code_row = bank_row * stride + slot_row
    shared_row = jnp.where(over_row > 0.5, over_rank, -1)

    def gathered(wanted, at):
        pick = jnp.where(wanted == at, 1.0, 0.0).astype(BF16)
        return jnp.dot(pick, tok[...], preferred_element_type=F32).astype(BF16)

    def fill(bank, height):
        return gathered(lax.broadcasted_iota(count, (height, rows), 0) + bank * stride, code_row)

    loads[2].wait()
    shared_out[...] = gathered(lax.broadcasted_iota(count, (shared, rows), 0), shared_row)
    pl.semaphore_wait(barrier, n - 1 + 2 * (m - 1))

    def send_idx(mask, _):
        idx_copy(mask, me).start()
        return 0

    lax.fori_loop(1, n, send_idx, 0)
    shared_first().start()
    loads[1].wait()

    @pl.when(inner)
    def _():
        up_copy(*own_across).start()

    up_copy(*own_side).start()

    def send_near(mask, _):
        outgoing[mask] = fill(partner(mask), near_rows)
        row_copy(mask, near_rows).start()
        return 0

    def send_far(mask, _):
        outgoing[mask, pl.ds(0, direct)] = fill(partner(mask), direct)
        row_copy(mask, direct).start()
        return 0

    lax.fori_loop(side, side + 1, send_near, 0)
    lax.fori_loop(1, 2, send_near, 0)

    def rs_copy(q):
        hop = low_bit(q)
        return pltpu.make_async_remote_copy(
            src_ref=rs_send.at[q], dst_ref=rs_recv.at[q],
            send_sem=rs_send_sem.at[q], recv_sem=rs_recv_sem.at[q],
            device_id={"ba": xor_bit(mb, hop)}, device_id_type=MESH,
        )

    loads[3].wait()
    loads[4].wait()
    base_order = sorted(range(1, m), key=lambda q: (low_bit(q), q)) + [0]

    def base(t, _):
        q = chosen(base_order, t)
        block = mb
        for b in ba_bits:
            block = jnp.where(lax.rem(q // b, 2) == 1, xor_bit(block, b), block)
        cols = pl.ds(pl.multiple_of(block * kv, LANES), kv)
        rs_send[q, :, :kv] = jnp.dot(tok[...], kw[:, cols], preferred_element_type=F32)
        rs_send[q, :, kv:] = jnp.dot(tok[...], vw[:, cols], preferred_element_type=F32)
        for at, q_now in enumerate(base_order):
            if q_now:
                @pl.when(t == at)
                def _():
                    for b in ba_bits:
                        if b < low_bit(q_now):
                            rs_copy(q_now + b).wait_recv()
                            rs_send[q_now] += rs_recv[q_now + b]
                    rs_copy(q_now).start()

        return 0

    lax.fori_loop(0, m, base, 0)

    idx_all[me] = row
    for_self = fill(me, near_rows)
    recv[0, pl.ds(0, near_rows)] = for_self
    for mask in range(half):
        recv[mask, pl.ds(near_rows, slots - near_rows)] = jnp.zeros((slots - near_rows, tok.shape[1]), BF16)

    landed(idx_all.at[pl.ds(0, n - 1)], idx_recv_sem.at[0])
    everyone = jnp.concatenate([idx_all[s] for s in range(n)], axis=0)
    banks = everyone // resident
    matches = [banks == b for b in range(n)]
    stacked = jnp.concatenate([jnp.where(hit, 1.0, 0.0) for hit in matches], axis=0)
    all_ranks = jnp.dot(stacked.astype(BF16), tri[...], preferred_element_type=F32)
    place = jnp.zeros((n, rows), F32)
    for b in range(n):
        place = place + jnp.where(matches[b], all_ranks[b * n:(b + 1) * n], 0.0)
    place = place.astype(count)
    far_all = (banks // half) != (lax.broadcasted_iota(count, (n, rows), 0) // half)
    over_all = jnp.where(far_all & (place >= direct), 1.0, 0.0)
    padded = jnp.concatenate([over_all] * (tall // n), axis=0)
    over_ranks = jnp.dot(padded.astype(BF16), tri[...], preferred_element_type=F32)[:n].astype(count)
    place = jnp.where(over_all > 0.5, direct + over_ranks, place)
    excess = jnp.where(place >= jnp.where(far_all, slots, near_rows), 1, 0)
    flag[0] = jnp.max(excess)
    flag_copy = pltpu.make_async_copy(flag, flag_hbm, store_sem.at[0])
    flag_copy.start()
    to_me = jnp.where(banks == me, place, -1)
    for s in range(n):
        mine[s] = to_me[s:s + 1]
    code_col = jnp.sum(jnp.where(earlier == later, code_row, 0), axis=1, keepdims=True)

    lane = lax.broadcasted_iota(count, (packed, LANES), 1) // twice_rank
    column = lax.broadcasted_iota(count, (slots, width), 1)
    for_key = lax.rem(column, twice_rank) < rank

    def folded(x):
        total = x
        for g in range(1, groups):
            total = total + pltpu.roll(x, g * twice_rank, axis=1)
        return total

    def owned(wanted, at, ids):
        local = jnp.sum(jnp.where(wanted == at, lax.rem(ids, resident), 0), axis=1, keepdims=True)
        return local == column // twice_rank

    def part_copy(b, mask):
        return pltpu.make_async_remote_copy(
            src_ref=rank_part.at[mask], dst_ref=rank_in.at[mask, b],
            send_sem=p_send_sem.at[mask], recv_sem=p_recv_sem.at[mask],
            device_id={"ba": lax.rem(mb + b + 1, m)}, device_id_type=MESH,
        )

    def direct_copy(b):
        return pltpu.make_async_remote_copy(
            src_ref=rank_part.at[half + 1], dst_ref=direct_in.at[b],
            send_sem=x_send_sem.at[0], recv_sem=x_recv_sem.at[0],
            device_id={"aa": partner(half + 1), "ba": lax.rem(mb + b, m)}, device_id_type=MESH,
        )

    def goes_direct(mask):
        return mask == half + 1

    def ret_copy(mask):
        return pltpu.make_async_remote_copy(
            src_ref=ret_send.at[mask], dst_ref=ret_recv.at[mask],
            send_sem=r_send_sem.at[mask], recv_sem=r_recv_sem.at[mask],
            device_id={"aa": partner(mask)}, device_id_type=MESH,
        )

    def partial(mask):
        @pl.when((mask > 0) & (mask < half))
        def _():
            row_copy(mask, near_rows).wait_recv()

        @pl.when(mask >= half)
        def _():
            row_copy(mask, direct).wait_recv()

        source = partner(mask)
        wide = jnp.dot(recv[mask], down_t[...], preferred_element_type=F32)
        own = owned(lax.broadcasted_iota(count, (slots, rows), 0), mine[source], idx_all[source])
        wide = jnp.where(own, wide, 0.0)
        total = wide[:, :LANES]
        for q in range(1, width // LANES):
            total = total + wide[:, q * LANES:(q + 1) * LANES]
        total = folded(total)
        if groups * packed > slots:
            total = jnp.concatenate([total, jnp.zeros((groups * packed - slots, LANES), F32)], axis=0)
        together = total[:packed]
        for g in range(1, groups):
            together = jnp.where(lane == g, total[g * packed:(g + 1) * packed], together)
        rank_part[mask] = together

        @pl.when(jnp.logical_not(goes_direct(mask) & outer))
        def _():
            for b in range(m - 1):
                part_copy(b, mask).start()

        @pl.when(goes_direct(mask) & outer)
        def _():
            for b in range(m):
                direct_copy(b).start()

    def finish(mask):
        total = rank_part[mask]
        landed(rank_in.at[mask], p_recv_sem.at[mask])
        for b in range(m - 1):
            total = total + rank_in[mask, b]

        @pl.when(mask == 0)
        def _():
            ret_recv[mask] = total

        @pl.when(mask > 0)
        def _():
            ret_send[mask] = total
            ret_copy(mask).start()

    def final(mask):
        @pl.when((mask > 0) & jnp.logical_not(goes_direct(mask) & inner))
        def _():
            ret_copy(mask).wait_recv()

        @pl.when(goes_direct(mask) & inner)
        def _():
            total = jnp.zeros((packed, LANES), F32)
            landed(direct_in, x_recv_sem.at[0])
            for b in range(m):
                total = total + direct_in[b]
            ret_recv[half + 1] = total

        bank = partner(mask)
        together = ret_recv[mask]
        tall_ranks = jnp.concatenate(
            [folded(jnp.where(lane == g, together, 0.0)) for g in range(groups)], axis=0
        )[:slots]
        own = owned(lax.broadcasted_iota(count, (slots, rows), 0) + bank * stride, code_row, row)
        spread = jnp.where(own, jnp.concatenate([tall_ranks] * (width // LANES), axis=1), 0.0)
        key_hi, key_lo = split_two(jnp.where(for_key, spread, 0.0))
        value_hi, value_lo = split_two(jnp.where(for_key, 0.0, spread))
        pieces = jnp.concatenate([key_hi, key_lo, value_hi, value_lo], axis=0)
        out = jnp.dot(pieces, up_all[mask], preferred_element_type=F32)
        change = jnp.concatenate(
            [out[:slots] + out[slots:2 * slots], out[2 * slots:3 * slots] + out[3 * slots:]], axis=1
        )
        hi, lo = split_two(change)
        pick = jnp.where(
            lax.broadcasted_iota(count, (rows, slots), 1) + bank * stride == code_col, 1.0, 0.0
        ).astype(BF16)
        acc[...] += jnp.dot(pick, hi, preferred_element_type=F32) + jnp.dot(
            pick, lo, preferred_element_type=F32
        )


    def line_up(q):
        up_arrived(q)

        @pl.when(inner)
        def _():
            up_copy(*line_copies[q]).start()

    def pair_up(q):
        up_copy(*pair_copies[q]).start()

    def pair_shared(q):
        shared_arrived(q)
        shared_pair(q).start()

    def init():
        for b in ba_bits:
            rs_copy(b).wait_recv()
            rs_send[0] += rs_recv[b]
        acc[...] = rs_send[0]

    two, three, four, five, six, seven = side, side + 1, half, half + 1, across, across + 1
    inner_turns = [
        (0, 0), (0, 1),
        (0, two), (0, four), (0, five), (1, 0), (2, 0), (1, 1), (1, two), (1, four), (1, five), (3, four),
        (0, three), (0, six), (1, three), (0, seven), (1, six), (2, 1), (1, seven), (3, five), (2, two), (2, three),
        (2, six), (2, seven), (2, four), (2, five),
    ]
    outer_turns = [
        (0, 0), (0, 1),
        (0, two), (1, 0), (2, 0), (1, 1), (1, two), (0, three), (0, six), (1, three), (0, seven), (1, six),
        (2, 1), (1, seven), (2, two), (2, four), (0, four), (2, three), (1, four), (2, five), (2, six), (0, five),
        (2, seven), (4, 0), (4, 0), (4, 0),
    ]
    opening = 2

    def turn(t, _):
        kind = jnp.where(inner, chosen([k for k, _ in inner_turns], t), chosen([k for k, _ in outer_turns], t))
        mask = jnp.where(inner, chosen([q for _, q in inner_turns], t), chosen([q for _, q in outer_turns], t))

        @pl.when((kind == 1) & (mask == 0) & outer)
        def _():
            pair_shared(across)
            pair_shared(half)

        for q in (half + 1, across + 1):
            @pl.when((kind == 0) & (mask == q))
            def _():
                shared_arrived(q)

        @pl.when((kind == 1) & (mask == jnp.where(inner, half, side + 1)))
        def _():
            line_up(half)
            pair_up(half)

        @pl.when((kind == 2) & (mask == 1) & outer)
        def _():
            line_up(across)
            pair_up(across)

        @pl.when((kind == 2) & (mask == 0))
        def _():
            init()

        for q in range(1, n, 2):
            @pl.when((kind == 2) & (mask == q))
            def _():
                up_arrived(q)

        @pl.when(kind == 0)
        def _():
            partial(mask)

        @pl.when(kind == 1)
        def _():
            finish(mask)

        @pl.when(kind == 2)
        def _():
            final(mask)

        @pl.when(kind == 3)
        def _():
            send_far(mask, 0)

        return 0

    @pl.when(inner)
    def _():
        for q in (half, across):
            shared_arrived(q)
            shared_line(q).start()
            shared_pair(q).start()

    line_up(side)
    lax.fori_loop(0, 2, lambda t, _: send_far(nearest + t, 0), 0)
    lax.fori_loop(side + 1, side + 2, send_near, 0)

    @pl.when(outer)
    def _():
        lax.fori_loop(across, across + 2, send_far, 0)

    up_copy(*own_pair).start()
    pair_up(side)
    loads[5].wait()

    def turn_down(c, _):
        strip = pl.ds(pl.multiple_of(c * LANES * 2, LANES), LANES * 2)
        down_t[strip] = down[:, strip].T
        return 0

    lax.fori_loop(0, down.shape[1] // (2 * LANES), turn_down, 0)
    lax.fori_loop(0, opening, turn, 0)

    @pl.when(inner)
    def _():
        line_up(across)
        pair_up(across)

    lax.fori_loop(opening, len(inner_turns), turn, 0)
    out[...] = acc[...].astype(BF16)

    shared_first().wait_send()
    for copy in (own_side, own_pair, *pair_copies.values()):
        up_copy(*copy).wait_send()
    for q in (half, across):
        shared_pair(q).wait_send()

    @pl.when(inner)
    def _():
        for copy in (own_across, *line_copies.values()):
            up_copy(*copy).wait_send()
        for q in (half, across):
            shared_line(q).wait_send()

    landed(idx_all.at[pl.ds(0, n - 1)], idx_send_sem.at[0])

    def drain(mask, _):
        @pl.when(jnp.logical_not(goes_direct(mask) & outer))
        def _():
            ret_copy(mask).wait_send()

        @pl.when(mask < half)
        def _():
            row_copy(mask, near_rows).wait_send()

        @pl.when(mask >= half)
        def _():
            row_copy(mask, direct).wait_send()

        return 0

    lax.fori_loop(1, n, drain, 0)

    def drain_parts(mask, _):
        @pl.when(jnp.logical_not(goes_direct(mask) & outer))
        def _():
            landed(rank_in.at[mask], p_send_sem.at[mask])

        return 0

    lax.fori_loop(0, n, drain_parts, 0)

    @pl.when(outer)
    def _():
        landed(direct_in, x_send_sem.at[0])

    for q in range(1, m):
        rs_copy(q).wait_send()
    flag_copy.wait()


def packed_call(n, m, cap, idx, tokens, key_weight, value_weight, down_flat, up_flat, resident):
    rows, width = tokens.shape
    flat = down_flat.shape[0]
    twice_rank = flat // resident
    kv_width = key_weight.shape[1]
    kv = kv_width // m
    direct = rows // n
    shared = 5 * direct // 8
    near_rows = 3 * direct // 2
    slots = direct + shared
    stride = resident * cap
    packed = stride * twice_rank // LANES
    dma = pltpu.SemaphoreType.DMA
    return pl.pallas_call(
        functools.partial(packed_kernel, n, m, direct, shared, near_rows, stride, resident, twice_rank),
        out_shape=[
            jax.ShapeDtypeStruct((rows, 2 * kv), BF16),
            jax.ShapeDtypeStruct((1,), jnp.int32),
        ],
        in_specs=[pl.BlockSpec(memory_space=pltpu.HBM)] * 6,
        out_specs=[pl.BlockSpec(memory_space=pltpu.VMEM), pl.BlockSpec(memory_space=pltpu.HBM)],
        scratch_shapes=[
            pltpu.VMEM((1, rows), jnp.int32),
            pltpu.VMEM((n, 1, rows), jnp.int32),
            pltpu.VMEM((n, 1, rows), jnp.int32),
            pltpu.VMEM((rows, rows), BF16),
            pltpu.VMEM((rows, width), BF16),
            pltpu.VMEM((width, kv_width), BF16),
            pltpu.VMEM((width, kv_width), BF16),
            pltpu.VMEM((flat, width), BF16),
            pltpu.VMEM((width, flat), BF16),
            pltpu.VMEM((n, flat, kv), BF16),
            pltpu.VMEM((shared, width), BF16),
            pltpu.VMEM((n, near_rows, width), BF16),
            pltpu.VMEM((n, slots, width), BF16),
            pltpu.VMEM((m, rows, 2 * kv), F32),
            pltpu.VMEM((m, rows, 2 * kv), F32),
            pltpu.VMEM((rows, 2 * kv), F32),
            pltpu.SMEM((1,), jnp.int32),
            pltpu.VMEM((n, packed, LANES), F32),
            pltpu.VMEM((n, m - 1, packed, LANES), F32),
            pltpu.VMEM((m, packed, LANES), F32),
            pltpu.VMEM((n, packed, LANES), F32),
            pltpu.VMEM((n, packed, LANES), F32),
            dma((6,)), dma((1,)), dma((1,)), dma((1,)),
            dma((1,)), dma((1,)), dma((10,)), dma((n,)), dma((5,)), dma((n,)),
            dma((n,)), dma((n,)),
            dma((m,)), dma((m,)),
            dma((n,)), dma((n,)),
            dma((n,)), dma((n,)),
        ],
        compiler_params=pltpu.CompilerParams(
            collective_id=1, has_side_effects=True, vmem_limit_bytes=63 * 1024 * 1024
        ),
    )(idx, tokens, key_weight, value_weight, down_flat, up_flat)


def on_device(n, m, tokens, request_adapter_index, key_weight, value_weight, down_weight, up_weight):
    rows, width = tokens.shape
    resident, twice_rank, _ = down_weight.shape
    kv_width = key_weight.shape[1]
    kv = kv_width // m
    cap = max(2, 2 * rows // (resident * n))
    chunk = resident * cap
    packed = chunk * twice_rank // LANES
    flat = resident * twice_rank
    operands = (
        request_adapter_index.reshape(1, rows),
        tokens,
        key_weight,
        value_weight,
        down_weight.reshape(flat, width),
        up_weight.reshape(flat, kv_width),
    )

    def any_load():
        dma = pltpu.SemaphoreType.DMA
        total = pl.pallas_call(
            functools.partial(kernel, n, m, cap, resident, twice_rank),
            out_shape=jax.ShapeDtypeStruct((rows, 2 * kv), F32),
            in_specs=[pl.BlockSpec(memory_space=pltpu.VMEM)] + [pl.BlockSpec(memory_space=pltpu.HBM)] * 5,
            out_specs=pl.BlockSpec(memory_space=pltpu.VMEM),
            scratch_shapes=[
                pltpu.VMEM((rows, width), BF16),
                pltpu.VMEM((width, kv_width), BF16),
                pltpu.VMEM((width, kv_width), BF16),
                pltpu.VMEM((flat, width), BF16),
                pltpu.VMEM((n, flat, kv), BF16),
                pltpu.VMEM((n, chunk, width), BF16),
                pltpu.VMEM((n, chunk, width), BF16),
                pltpu.VMEM((m, rows, 2 * kv), F32),
                pltpu.VMEM((m - 1, rows, 2 * kv), F32),
                pltpu.VMEM((n, packed, LANES), F32),
                pltpu.VMEM((m - 1, n, packed, LANES), F32),
                pltpu.VMEM((n, packed, LANES), F32),
                pltpu.VMEM((n, packed, LANES), F32),
                dma((5,)),
                dma((n,)), dma((n,)), dma((n,)), dma((n,)),
                dma((m,)), dma((m,)),
                dma((m - 1, n)), dma((m - 1, n)),
                dma((n,)), dma((n,)),
            ],
            compiler_params=pltpu.CompilerParams(
                collective_id=0, has_side_effects=True, vmem_limit_bytes=56 * 1024 * 1024
            ),
        )(
            *operands,
        )
        return total.astype(BF16)

    if n // 2 != 4 or rows % (64 * n) or 13 * rows // (8 * n) >= chunk:
        both = any_load()
    else:
        both, flag = packed_call(n, m, cap, *operands, resident)
        both = lax.cond(flag.reshape(()) > 0, any_load, lambda: both)
    return both[:, :kv], both[:, kv:]


def solution(mesh):
    return jax.shard_map(
        functools.partial(on_device, mesh.shape["aa"], mesh.shape["ba"]),
        mesh=mesh,
        in_specs=(
            P("aa", "ba"),
            P("aa", None),
            P("ba", None),
            P("ba", None),
            P("aa", None, "ba"),
            P("aa", None, None, None),
        ),
        out_specs=(P("aa", "ba"), P("aa", "ba")),
        check_vma=False,
    )
```
